32 devices in a mesh: gx: 8 (over z, x), gy: 4 (over y, core).
Axes of the slice: x: 2, y: 2, z: 4, core: 2. Of those that a mesh axis runs over, the one named last changes fastest.
Arguments:
- density: float32 [512, 128, 128], P('gx', 'gy'), may hold values from -6 to 6
- slowness: float32 [512, 128, 128], P('gx', 'gy'), may hold values from -6 to 6
- pressure_obs: float32 [512, 128, 128], P('gx', 'gy'), may hold values from -6 to 6
- time_obs: float32 [512, 128, 128], P('gx', 'gy'), may hold values from -6 to 6
- zone_map: int32 [512, 128, 128], P('gx', 'gy'), may hold values from 0 to 7
- zone_low: float32 [8], replicated, may hold values from -2.5 to -0.5
- zone_high: float32 [8], replicated, may hold values from 0.5 to 2.5
Outputs:
- density_out: float32 [512, 128, 128], P('gx', 'gy')
- slowness_out: float32 [512, 128, 128], P('gx', 'gy')
- objective: float32 [3], replicated
The draws below stay inside these ranges and needn't reach their ends.
All inputs are finite; a program needn't handle non-finite values.
Results may differ from the reference program's by a relative error of at most 0.00013.
Values sent between devices are 32-bit elements; how exact they have to be, the bound alone decides.
A program may use at most 128 MiB of HBM per device.

```python
import jax
import jax.numpy as jnp
from jax import lax

ITERS = 3
ZONES = 8
NX = 512
NY = 128
NZ = 128


def with_ends(array, own_key, low, top_value):
    shape = array.shape
    spot = [jax.random.randint(jax.random.fold_in(own_key, axis), (), 0, shape[axis]) for axis in range(len(shape))]
    array = array.at[tuple(spot)].set(low)
    longest = shape.index(max(shape))
    spot[longest] = (spot[longest] + 1) % shape[longest]
    return array.at[tuple(spot)].set(top_value)


def block_scale(stream_key, shape, split, least, top_value):
    level = 1.0
    for axis_at, parts in split:
        draws = jax.random.uniform(jax.random.fold_in(jax.random.fold_in(stream_key, 6), axis_at), (parts,), jnp.float32, least / len(split), top_value / len(split))
        level = level * jnp.repeat(jnp.exp(draws), shape[axis_at] // parts).reshape((-1,) + (1,) * (len(shape) - 1 - axis_at))
    return level


def normal_values(stream_key, dims, spread, bound, pieces=(), held_as=jnp.bfloat16):
    entries = jax.random.normal(stream_key, dims, jnp.float32) * spread
    if len(pieces) > 0:
        entries = block_scale(stream_key, dims, pieces, -0.22, 0.18) * entries
    return jnp.clip(entries, min=-bound, max=bound).astype(held_as)


def setup_inputs(seed: int = 0) -> dict:
    splits = jax.random.split(jax.random.key(seed), 8)
    return {
        "density": normal_values(splits[0], (NX, NY, NZ), 1.0, 6.0, ((0, 8), (1, 4)), jnp.float32),
        "slowness": normal_values(splits[1], (NX, NY, NZ), 1.0, 6.0, ((0, 8), (1, 4)), jnp.float32),
        "pressure_obs": normal_values(splits[2], (NX, NY, NZ), 1.0, 6.0, ((0, 8), (1, 4)), jnp.float32),
        "time_obs": normal_values(splits[3], (NX, NY, NZ), 1.0, 6.0, ((0, 8), (1, 4)), jnp.float32),
        "zone_map": with_ends(jax.random.randint(splits[4], (NX, NY, NZ), 0, ZONES), jax.random.fold_in(splits[4], 1), 0, ZONES - 1).astype(jnp.int32),
        "zone_low": jnp.clip(jax.random.uniform(splits[5], (ZONES,), jnp.float32, -2.5, -0.5), -2.5, -0.5),
        "zone_high": jnp.clip(jax.random.uniform(splits[6], (ZONES,), jnp.float32, 0.5, 2.5), 0.5, 2.5),
    }


BETA = 1.0
ETA = 0.5
EPSILON = 1e-06

def slopes(field):
    padded = jnp.pad(field, 1)
    along_x = (padded[2:, 1:-1, 1:-1] - padded[:-2, 1:-1, 1:-1]) * 0.5
    along_y = (padded[1:-1, 2:, 1:-1] - padded[1:-1, :-2, 1:-1]) * 0.5
    along_z = (padded[1:-1, 1:-1, 2:] - padded[1:-1, 1:-1, :-2]) * 0.5
    return (along_x, along_y, along_z)

def slopes_adjoint(values):
    first = jnp.pad(values[0], 1)
    second = jnp.pad(values[1], 1)
    third = jnp.pad(values[2], 1)
    total = (first[:-2, 1:-1, 1:-1] - first[2:, 1:-1, 1:-1]) * 0.5
    total = total + (second[1:-1, :-2, 1:-1] - second[1:-1, 2:, 1:-1]) * 0.5
    total = total + (third[1:-1, 1:-1, :-2] - third[1:-1, 1:-1, 2:]) * 0.5
    return total

def cross_product(first_vec, second_vec):
    return (first_vec[1] * second_vec[2] - first_vec[2] * second_vec[1], first_vec[2] * second_vec[0] - first_vec[0] * second_vec[2], first_vec[0] * second_vec[1] - first_vec[1] * second_vec[0])

def reverse_cumsum(values, axis_number):
    return jnp.flip(jnp.cumsum(jnp.flip(values, axis_number), axis_number), axis_number)

def reference(density, slowness, pressure_obs, time_obs, zone_map, zone_low, zone_high):
    lower_bound = zone_low[zone_map]
    upper_bound = zone_high[zone_map]
    cells = float(NX * NY * NZ)
    zscale = 1.0 / float(NZ) ** 0.5
    xscale = 1.0 / float(NX) ** 0.5
    density_now = density
    slowness_now = slowness
    history = []
    for iteration in range(ITERS):
        first_vec = slopes(density_now)
        second_vec = slopes(slowness_now)
        crossed = cross_product(first_vec, second_vec)
        pressure_miss = jnp.cumsum(density_now, axis=2) * zscale - pressure_obs
        time_miss = jnp.cumsum(slowness_now, axis=0) * xscale - time_obs
        crossed_sq = jnp.sum(crossed[0] * crossed[0]) + jnp.sum(crossed[1] * crossed[1]) + jnp.sum(crossed[2] * crossed[2])
        history.append(0.5 * (jnp.sum(pressure_miss * pressure_miss) + jnp.sum(time_miss * time_miss) + BETA * crossed_sq) / cells)
        toward_density = cross_product(second_vec, crossed)
        toward_slowness = cross_product(crossed, first_vec)
        grad_density = reverse_cumsum(pressure_miss, 2) * zscale + BETA * slopes_adjoint(toward_density)
        grad_slowness = reverse_cumsum(time_miss, 0) * xscale + BETA * slopes_adjoint(toward_slowness)
        norm_density = jnp.sum(grad_density * grad_density)
        norm_slowness = jnp.sum(grad_slowness * grad_slowness)
        moved = density_now - ETA * grad_density * lax.rsqrt(norm_density / cells + EPSILON)
        density_now = jnp.minimum(jnp.maximum(moved, lower_bound), upper_bound)
        slowness_now = slowness_now - ETA * grad_slowness * lax.rsqrt(norm_slowness / cells + EPSILON)
    return (density_now, slowness_now, jnp.stack(history))
```

```python
import functools
import math

import jax
import jax.numpy as jnp
from jax import lax
from jax.experimental import pallas as pl
from jax.experimental.pallas import tpu as pltpu
from jax.sharding import PartitionSpec as P

ITERS = 3
BETA = 1.0
ETA = 0.5
EPSILON = 1e-06
MESH = pl.DeviceIdType.MESH
F32 = jnp.float32
BF16 = jnp.bfloat16


def split(v):
    hi = v.astype(BF16)
    lo = (v - hi.astype(F32)).astype(BF16)
    return jnp.concatenate([hi, lo], axis=-1)


def kernel(
    nx, ny,
    zlow_h, zhigh_h, rho_h, sig_h, p_h, t_h, zone_h,
    rho, sig, grho, gsig, low, high, stat,
    zlow, zhigh, p, t, zone, gp, lin,
    u1, v1, u2, v2, e3, f3, da, db, dedge, wts, ltab,
    rim, rim2, ysend, yrecv, xrecv, csend, crecv, pwsend, pwrecv, before, zsum, nsend, nrecv,
    insem, ys, yr, xs_, xr, cs, cr, ps, pr, ns, nr,
):
    X, Y, Z = p.shape
    mx, my = lax.axis_index("gx"), lax.axis_index("gy")
    n = nx * ny
    me = mx * ny + my
    N = nx * X
    cells = float(N * ny * Y * Z)
    zscale = 1.0 / math.sqrt(Z)
    xscale = 1.0 / math.sqrt(N)
    R = pl.ds(8, Y)
    i0 = (mx * X).astype(F32)

    inner = (pl.ds(2, X), R)
    loads = [
        pltpu.make_async_copy(sig_h, sig.at[inner], insem.at[0]),
        pltpu.make_async_copy(rho_h, rho.at[inner], insem.at[1]),
        pltpu.make_async_copy(t_h, t, insem.at[2]),
        pltpu.make_async_copy(zone_h, zone, insem.at[3]),
        pltpu.make_async_copy(p_h, p, insem.at[4]),
        pltpu.make_async_copy(zlow_h, zlow, insem.at[5]),
        pltpu.make_async_copy(zhigh_h, zhigh, insem.at[6]),
    ]
    for c in loads:
        c.start()
    barrier = pltpu.get_barrier_semaphore()

    has = {0: (mx > 0, my > 0), 1: (mx < nx - 1, my < ny - 1)}

    def zero_y(s):
        @pl.when(jnp.logical_not(has[s][1]))
        def _():
            for r in range(4):
                yrecv[r, s] = jnp.zeros(yrecv.shape[2:], F32)

    def zero_x(s):
        @pl.when(jnp.logical_not(has[s][0]))
        def _():
            for r in range(4):
                xrecv[r, s] = jnp.zeros(xrecv.shape[2:], F32)

    def other(dx, dy):
        tx = lax.rem(mx + dx, nx) if dx else mx
        ty = lax.rem(my + dy, ny) if dy else my
        return tx, ty

    pairs = [(dx, dy) for dx in range(nx) for dy in range(ny)][1:]
    for dx, dy in pairs:
        pl.semaphore_signal(barrier, inc=1, device_id=other(dx, dy), device_id_type=MESH)

    for s in range(2):
        zero_y(s)
        zero_x(s)
    for sx in range(2):
        for sy in range(2):
            @pl.when(jnp.logical_not(jnp.logical_and(has[sx][0], has[sy][1])))
            def _():
                for r in range(4):
                    crecv[r, sx, sy] = jnp.zeros((8, Z), F32)
    csend[...] = jnp.zeros(csend.shape, F32)

    def ycopy(r, s):
        b = 1 if r == 3 else 0
        return pltpu.make_async_remote_copy(
            src_ref=ysend.at[b, s], dst_ref=yrecv.at[r, 1 - s],
            send_sem=ys.at[r, s], recv_sem=yr.at[r, 1 - s],
            device_id=(mx, my + (2 * s - 1)), device_id_type=MESH)

    def xsource(r, s, f):
        if r == 0:
            src = (rho, sig)[f]
            return src.at[pl.ds(2 + s * (X - 2), 2), R]
        src = ((low, high) if r == 3 else (grho, gsig))[f]
        return src.at[pl.ds(s * (X - 2), 2)]

    def xcopy(r, s, f):
        return pltpu.make_async_remote_copy(
            src_ref=xsource(r, s, f), dst_ref=xrecv.at[r, 1 - s, f],
            send_sem=xs_.at[r, s, f], recv_sem=xr.at[r, 1 - s, f],
            device_id=(mx + (2 * s - 1), my), device_id_type=MESH)

    def ccopy(r, sx, sy):
        b = 1 if r == 3 else 0
        return pltpu.make_async_remote_copy(
            src_ref=csend.at[b, sx, sy], dst_ref=crecv.at[r, 1 - sx, 1 - sy],
            send_sem=cs.at[r, sx, sy], recv_sem=cr.at[r, 1 - sx, 1 - sy],
            device_id=(mx + (2 * sx - 1), my + (2 * sy - 1)), device_id_type=MESH)

    def rims_start(r):
        for s in range(2):
            @pl.when(has[s][1])
            def _():
                ycopy(r, s).start()

            @pl.when(has[s][0])
            def _():
                for f in range(2):
                    xcopy(r, s, f).start()
        for sx in range(2):
            for sy in range(2):
                @pl.when(jnp.logical_and(has[sx][0], has[sy][1]))
                def _():
                    ccopy(r, sx, sy).start()

    def yrims_wait(r):
        for s in range(2):
            @pl.when(has[s][1])
            def _():
                ycopy(r, 1 - s).wait_recv()
                ycopy(r, s).wait_send()
        for sx in range(2):
            for sy in range(2):
                @pl.when(jnp.logical_and(has[sx][0], has[sy][1]))
                def _():
                    ccopy(r, 1 - sx, 1 - sy).wait_recv()
                    ccopy(r, sx, sy).wait_send()

    def xrims_wait(r):
        for s in range(2):
            @pl.when(has[s][0])
            def _():
                for f in range(2):
                    xcopy(r, 1 - s, f).wait_recv()
                    xcopy(r, s, f).wait_send()

    def pwcopy(r, tx, slot):
        later = jnp.where(tx > mx, 0, 1)
        return pltpu.make_async_remote_copy(
            src_ref=pwsend.at[later], dst_ref=pwrecv.at[r, slot],
            send_sem=ps.at[r, tx], recv_sem=pr.at[r, slot],
            device_id=(tx, my), device_id_type=MESH)

    def pw_start(r):
        for dx in range(1, nx):
            pwcopy(r, other(dx, 0)[0], mx).start()

    def pw_wait(r):
        def go(d, carry):
            tx = lax.rem(mx + d, nx)
            pwcopy(r, tx, tx).wait_recv()
            pwcopy(r, tx, tx).wait_send()
            return carry
        lax.fori_loop(1, nx, go, 0)

        def add(d, carry):
            a, b = carry
            tx = lax.rem(mx + d, nx)
            v = pwrecv[r, tx]
            w = jnp.where(tx < mx, 1.0, 0.0)
            return a + v * w, b + v * (1.0 - w)
        zero = jnp.zeros((Y, Z), F32)
        return lax.fori_loop(1, nx, add, (zero, zero))

    def n_start(r):
        for d, (dx, dy) in enumerate(pairs):
            pltpu.make_async_remote_copy(
                src_ref=nsend.at[r, pl.ds(0, 1)], dst_ref=nrecv.at[r, pl.ds(d, 1)],
                send_sem=ns.at[r], recv_sem=nr.at[r],
                device_id=other(dx, dy), device_id_type=MESH).start()

    def n_wait(r):
        rows = nrecv.at[r, pl.ds(0, n - 1)]
        every = pltpu.make_async_remote_copy(
            src_ref=rows, dst_ref=rows, send_sem=ns.at[r], recv_sem=nr.at[r],
            device_id=other(0, 1), device_id_type=MESH)
        every.wait_recv()
        every.wait_send()
        return jnp.sum(nrecv[r], axis=0, keepdims=True)

    def fold(v):
        out = v[0:8]
        for k in range(8, v.shape[0], 8):
            out = out + v[k:k + 8]
        return out

    def gather(b, f, x, v):
        row = pl.ds(x, 1)
        ysend[b, 0, f, 0, row, :] = v[0:1]
        ysend[b, 0, f, 1, row, :] = v[1:2]
        ysend[b, 1, f, 0, row, :] = v[Y - 1:Y]
        ysend[b, 1, f, 1, row, :] = v[Y - 2:Y - 1]

    def corners(b, f):
        for sx in range(2):
            for sy in range(2):
                csend[b, sx, sy, f:f + 1, :] = ysend[b, sy, f, 0, sx * (X - 1):sx * (X - 1) + 1, :]

    zero = jnp.zeros((Y, Z), F32)

    with jax.named_scope("load02"):
        loads[0].wait()
        loads[2].wait()

    def sums(x, carry):
        a, b, c = carry
        v = sig[x + 2, R, :]
        gather(0, 1, x, v)
        weight = float(N) - i0 - x.astype(F32)
        return a + v, b + weight * v, c + t[x]

    psum_, wsum, tsum = lax.fori_loop(0, X, sums, (zero, zero, zero), unroll=4)
    zown = xscale * wsum - tsum
    pwsend[0] = psum_
    pwsend[1] = zown
    loads[1].wait()

    def copy_rho(x, carry):
        gather(0, 0, x, rho[x + 2, R, :])
        return carry

    lax.fori_loop(0, X, copy_rho, 0, unroll=4)
    corners(0, 0)
    corners(0, 1)
    with jax.named_scope("barrier"):
        pl.semaphore_wait(barrier, n - 1)
    rims_start(0)
    pw_start(0)

    for c in loads[3:]:
        c.wait()

    def bounds(x, carry):
        ids = zone[x]
        lo = jnp.zeros((Y, Z), F32)
        hi = jnp.zeros((Y, Z), F32)
        for k in range(zlow.shape[0]):
            hit = ids == k
            lo = jnp.where(hit, zlow[k], lo)
            hi = jnp.where(hit, zhigh[k], hi)
        low[x] = lo
        high[x] = hi
        gather(1, 0, x, lo)
        gather(1, 1, x, hi)
        return carry

    lax.fori_loop(0, X, bounds, 0, unroll=2)
    corners(1, 0)
    corners(1, 1)

    ri = lax.broadcasted_iota(jnp.int32, (Z, Z), 0)
    ci = lax.broadcasted_iota(jnp.int32, (Z, Z), 1)
    m = (Z - jnp.maximum(ri, ci)).astype(F32).astype(BF16)
    u = jnp.where(ri <= ci, 1.0, 0.0).astype(BF16)
    l = jnp.where(ri >= ci, 1.0, 0.0).astype(BF16)
    band = jnp.where(ri == ci + 1, 1.0, jnp.where(ri == ci - 1, -1.0, 0.0)).astype(BF16)
    for half in (slice(0, Z), slice(Z, 2 * Z)):
        wts[half, 0:Z] = m
        wts[half, Z:2 * Z] = band
        wts[half, 2 * Z:3 * Z] = u
    ltab[0:Z] = l
    ltab[Z:2 * Z] = l

    block = X
    band2 = wts.at[:, pl.ds(Z, Z)]

    def slope(v):
        return jnp.dot(split(v), band2[...], preferred_element_type=F32)


    def pback(k, carry):
        rows = pl.ds(k * block, block)
        v = p[rows].reshape(block * Y, Z)
        out = jnp.dot(split(v), ltab[...], preferred_element_type=F32)
        gp[rows] = (out * zscale).reshape(block, Y, Z)
        return carry

    lax.fori_loop(0, X // block, pback, 0)

    def zlin(k, carry):
        v = rho[pl.ds(2 + k * block, block), R, :].reshape(block * Y, Z)
        out = jnp.dot(split(v), wts[...], preferred_element_type=F32)
        rows = pl.ds(k * block, block)
        lin[rows] = out[:, 0:Z].reshape(block, Y, Z)
        da[rows] = out[:, Z:2 * Z].reshape(block, Y, Z)
        rp = zscale * out[:, 2 * Z:3 * Z].reshape(block, Y, Z) - p[rows]
        v = sig[pl.ds(2 + k * block, block), R, :].reshape(block * Y, Z)
        db[rows] = slope(v).reshape(block, Y, Z)
        return carry + fold((rp * rp).reshape(block * Y, Z))

    def zadj(k, carry):
        rows = pl.ds(k * block, block)
        for a in (e3, f3):
            a[rows] = slope(a[rows].reshape(block * Y, Z)).reshape(block, Y, Z)
        return carry

    def edges():
        dedge[...] = slope(jnp.concatenate(
            [rim[f, s, 1, XI, :] for f in range(2) for s in range(2)], axis=0))

    def xedges():
        return slope(jnp.concatenate(
            [a[x, R, :] for a in (rho, sig) for x in (1, X + 2)], axis=0))

    def set_rows(x, carry):
        for f, a in ((0, rho), (1, sig)):
            for s in range(2):
                a[x + 2, pl.ds(7 + s * (Y + 1), 1), :] = rim[f, s, 1, pl.ds(8 + x, 1), :]
        return carry

    def set_corners():
        for f, a in ((0, rho), (1, sig)):
            for sx in range(2):
                for sy in range(2):
                    a[1 + sx * (X + 1), pl.ds(7 + sy * (Y + 1), 1), :] = (
                        rim[f, sy, 1, 7 + sx * (X + 1):8 + sx * (X + 1), :])

    XI = pl.ds(8, X)

    for k in range(ITERS):
        if k == 0:
            with jax.named_scope("zlin"):
                psq = lax.fori_loop(0, X // block, zlin, jnp.zeros((8, Z), F32))
            with jax.named_scope("yrimwait"):
                yrims_wait(0)
            for f, a in ((0, rho), (1, sig)):
                for s in range(2):
                    rim[f, s, 0, XI, :] = yrecv[0, s, f, 1]
                    rim[f, s, 1, XI, :] = yrecv[0, s, f, 0]
                    rim[f, s, 2, XI, :] = ysend[0, s, f, 0]
                    for sx in range(2):
                        rim[f, s, 1, 7 + sx * (X + 1):8 + sx * (X + 1), :] = crecv[0, sx, s, f:f + 1, :]
        else:
            with jax.named_scope("yrimwait"):
                if k == 1:
                    yrims_wait(3)
                yrims_wait(k)
            for s in range(2):
                for row, slot in ((0, 1), (1, 0), (2, 0)):
                    gr = (ysend[0, s, 0, 0] if row == 2 else yrecv[k, s, 0, slot])
                    gs = (ysend[0, s, 1, 0] if row == 2 else yrecv[k, s, 1, slot])
                    lo = (ysend[1, s, 0, 0] if row == 2 else yrecv[3, s, 0, slot])
                    hi = (ysend[1, s, 1, 0] if row == 2 else yrecv[3, s, 1, slot])
                    rim[0, s, row, XI, :] = jnp.minimum(jnp.maximum(rim[0, s, row, XI, :] - step_r * gr, lo), hi)
                    rim[1, s, row, XI, :] = rim[1, s, row, XI, :] - step_s * gs
                for sx in range(2):
                    at = slice(7 + sx * (X + 1), 8 + sx * (X + 1))
                    rim[0, s, 1, at, :] = jnp.minimum(jnp.maximum(
                        rim[0, s, 1, at, :] - step_r * crecv[k, sx, s, 0:1, :],
                        crecv[3, sx, s, 0:1, :]), crecv[3, sx, s, 1:2, :])
                    rim[1, s, 1, at, :] = rim[1, s, 1, at, :] - step_s * crecv[k, sx, s, 1:2, :]
        with jax.named_scope("setrows"):
            lax.fori_loop(0, X, set_rows, 0, unroll=4)
            set_corners()
        if k > 0:
            with jax.named_scope("zlin"):
                psq = lax.fori_loop(0, X // block, zlin, jnp.zeros((8, Z), F32))
        with jax.named_scope("edges"):
            edges()

        for s in range(2):
            def rimstep(q, carry):
                base = pl.multiple_of(q * 8, 8)
                def vec(f):
                    a1 = rim[f, s, 1, pl.ds(9 + base, 8), :] - rim[f, s, 1, pl.ds(7 + base, 8), :]
                    a2 = rim[f, s, 2 - 2 * s, pl.ds(8 + base, 8), :] - rim[f, s, 2 * s, pl.ds(8 + base, 8), :]
                    return a1, a2, dedge[pl.ds((2 * f + s) * X + base, 8), :]
                a1, a2, a3 = vec(0)
                b1, b2, b3 = vec(1)
                c1 = a2 * b3 - a3 * b2
                c3 = a1 * b2 - a2 * b1
                rim2[s, 0, pl.ds(base, 8), :] = b3 * c1 - b1 * c3
                rim2[s, 1, pl.ds(base, 8), :] = c3 * a1 - c1 * a3
                return carry
            with jax.named_scope("rimstep"):
                lax.fori_loop(0, X // 8, rimstep, 0)

        def vectors(a, x, a3):
            a1 = a[x + 1, R, :] - a[x - 1, R, :]
            a2 = a[x, pl.ds(9, Y), :] - a[x, pl.ds(7, Y), :]
            return a1, a2, a3

        def edge(x, ds):
            at = Y if x > 1 else 0
            a1, a2, a3 = vectors(rho, x, ds[at:at + Y])
            b1, b2, b3 = vectors(sig, x, ds[at + 2 * Y:at + 3 * Y])
            c2 = a3 * b1 - a1 * b3
            c3 = a1 * b2 - a2 * b1
            u1[x - 1] = b2 * c3 - b3 * c2
            v1[x - 1] = c2 * a3 - c3 * a2

        def pass1(i, acc):
            x = i + 2
            a1, a2, a3 = vectors(rho, x, da[i])
            b1, b2, b3 = vectors(sig, x, db[i])
            c1 = a2 * b3 - a3 * b2
            c2 = a3 * b1 - a1 * b3
            c3 = a1 * b2 - a2 * b1
            u1[i + 1] = b2 * c3 - b3 * c2
            v1[i + 1] = c2 * a3 - c3 * a2
            u2[i, R, :] = b3 * c1 - b1 * c3
            v2[i, R, :] = c3 * a1 - c1 * a3
            e3[i] = b1 * c2 - b2 * c1
            f3[i] = c1 * a2 - c2 * a1
            for s in range(2):
                at = pl.ds(7 + s * (Y + 1), 1)
                u2[i, at, :] = rim2[s, 0, pl.ds(i, 1), :]
                v2[i, at, :] = rim2[s, 1, pl.ds(i, 1), :]
            return acc + fold(c1 * c1 + c2 * c2 + c3 * c3)

        with jax.named_scope("pass1"):
            csq = lax.fori_loop(2, X - 2, pass1, jnp.zeros((8, Z), F32), unroll=4)
            csq = pass1(1, csq)
            csq = pass1(X - 2, csq)
        with jax.named_scope("xrimwait"):
            if k == 1:
                xrims_wait(3)
            xrims_wait(k)
        for s in range(2):
            pls = pl.ds(s * (X + 2), 2)
            if k == 0:
                rho[pls, R, :] = xrecv[0, s, 0]
                sig[pls, R, :] = xrecv[0, s, 1]
            else:
                rho[pls, R, :] = jnp.minimum(jnp.maximum(
                    rho[pls, R, :] - step_r * xrecv[k, s, 0], xrecv[3, s, 0]), xrecv[3, s, 1])
                sig[pls, R, :] = sig[pls, R, :] - step_s * xrecv[k, s, 1]
        if k == 0:
            with jax.named_scope("rims3start"):
                rims_start(3)
        with jax.named_scope("edge"):
            ds = xedges()
            edge(1, ds)
            edge(X + 2, ds)
            csq = pass1(0, csq)
            csq = pass1(X - 1, csq)
        with jax.named_scope("zadj"):
            lax.fori_loop(0, X // block, zadj, 0)

        if k == 0:
            with jax.named_scope("pwwait"):
                a, b = pw_wait(0)
            before[...] = a
            zsum[...] = b + zown
        else:
            with jax.named_scope("pwwait"):
                a, b = pw_wait(k)
            before[...] = before[...] - step_s * a
            zsum[...] = zsum[...] - (step_s * xscale) * (b + wg)
        start = xscale * (float(N) - i0) * before[...] + zsum[...]

        def pass2(i, carry):
            pref, back, pg, wg, acc, nrho, nsig = carry
            v = sig[i + 2, R, :]
            pref = pref + v
            rt = xscale * pref - t[i]
            adj_s = (v1[i] - v1[i + 2]) + (v2[i, pl.ds(7, Y), :] - v2[i, pl.ds(9, Y), :]) - f3[i]
            gs = xscale * back + (BETA / 16.0) * adj_s
            back = back - rt
            adj_r = (u1[i] - u1[i + 2]) + (u2[i, pl.ds(7, Y), :] - u2[i, pl.ds(9, Y), :]) - e3[i]
            gr = (zscale * zscale) * lin[i] - gp[i] + (BETA / 16.0) * adj_r
            grho[i] = gr
            gsig[i] = gs
            acc = acc + fold(rt * rt)
            nrho = nrho + fold(gr * gr)
            nsig = nsig + fold(gs * gs)
            if k < ITERS - 1:
                gather(0, 0, i, gr)
                gather(0, 1, i, gs)
                pg = pg + gs
                wg = wg + (float(N) - i0 - i.astype(F32)) * gs
            return pref, back, pg, wg, acc, nrho, nsig

        z8 = jnp.zeros((8, Z), F32)
        with jax.named_scope("pass2"):
            _, _, pg, wg, acc, nrho, nsig = lax.fori_loop(
                0, X, pass2, (before[...], start, zero, zero, z8, z8, z8), unroll=2)
        local = (0.5 / cells) * (acc + psq + (BETA / 16.0) * csq)
        lane = lax.broadcasted_iota(jnp.int32, (1, Z), 1)

        def total(v):
            return jnp.sum(jnp.sum(v, axis=0, keepdims=True), axis=1, keepdims=True)

        row = jnp.where(lane < 1, total(nrho), jnp.where(lane < 2, total(nsig), total(local)))
        nsend[k, 0:1] = row
        nrecv[k, n - 1:n] = row
        with jax.named_scope("nstart"):
            n_start(k)
        if k < ITERS - 1:
            pwsend[0] = pg
            pwsend[1] = wg
            corners(0, 0)
            corners(0, 1)
        if k < ITERS - 1:
            with jax.named_scope("rimstart"):
                rims_start(k + 1)
                pw_start(k + 1)
        with jax.named_scope("nwait"):
            tot = n_wait(k)
        steps = ETA * lax.rsqrt(tot / cells + EPSILON)
        step_r = jnp.broadcast_to(steps[0:1, 0:1], (1, Z))
        step_s = jnp.broadcast_to(steps[0:1, 1:2], (1, Z))
        stat[k:k + 1, :] = jnp.broadcast_to(tot[0:1, 2:3], (1, Z))

        def update(i, carry):
            rho[i + 2, R, :] = jnp.minimum(jnp.maximum(rho[i + 2, R, :] - step_r * grho[i], low[i]), high[i])
            sig[i + 2, R, :] = sig[i + 2, R, :] - step_s * gsig[i]
            return carry

        if k < ITERS - 1:
            with jax.named_scope("update"):
                lax.fori_loop(0, X, update, 0, unroll=4)
        else:
            stat[ITERS:ITERS + 1, :] = step_r
            stat[ITERS + 1:ITERS + 2, :] = step_s


def finish(rho, sig, grho, gsig, low, high, stat, rho_o, sig_o, obj_o, rho_b, sig_b, obj, sems):
    X, Y, Z = grho.shape
    R = pl.ds(8, Y)
    seen = stat[...]
    for k in range(ITERS):
        obj[k] = seen[k, 0]
    copies = [pltpu.make_async_copy(obj, obj_o, sems.at[0])]
    copies[0].start()
    step_r = stat[ITERS:ITERS + 1, :]
    step_s = stat[ITERS + 1:ITERS + 2, :]

    def move(i, carry):
        rho_b[i] = jnp.minimum(jnp.maximum(rho[i + 2, R, :] - step_r * grho[i], low[i]), high[i])
        sig_b[i] = sig[i + 2, R, :] - step_s * gsig[i]
        return carry

    parts = 4
    for c in range(parts):
        lax.fori_loop(c * X // parts, (c + 1) * X // parts, move, 0, unroll=4)
        rows = pl.ds(c * X // parts, X // parts)
        for f, (a, b) in enumerate(((rho_b, rho_o), (sig_b, sig_o))):
            copies.append(pltpu.make_async_copy(a.at[rows], b.at[rows], sems.at[1 + 2 * c + f]))
            copies[-1].start()
    for c in copies:
        c.wait()


def local(density, slowness, pressure_obs, time_obs, zone_map, zone_low, zone_high):
    X, Y, Z = density.shape
    nx, ny = lax.axis_size("gx"), lax.axis_size("gy")
    assert Z <= 256
    V = pltpu.VMEM
    cube = (X, Y, Z)
    padded = (X + 4, Y + 16, Z)
    dma = pltpu.SemaphoreType.DMA
    anyspace = pl.BlockSpec(memory_space=pl.ANY)
    zones = zone_low.shape[0]
    scratch = [
        pltpu.SMEM((zones,), F32), pltpu.SMEM((zones,), F32),
        V(cube, F32), V(cube, F32),
        V(cube, jnp.int32), V(cube, F32), V(cube, F32),
        V((X + 2, Y, Z), F32), V((X + 2, Y, Z), F32), V((X, Y + 16, Z), F32), V((X, Y + 16, Z), F32),
        V(cube, F32), V(cube, F32), V(cube, F32), V(cube, F32), V((4 * X, Z), F32),
        V((2 * Z, 3 * Z), BF16), V((2 * Z, Z), BF16),
        V((2, 2, 3, X + 16, Z), F32), V((2, 2, X, Z), F32),
        V((2, 2, 2, 2, X, Z), F32), V((4, 2, 2, 2, X, Z), F32), V((4, 2, 2, 2, Y, Z), F32),
        V((2, 2, 2, 8, Z), F32), V((4, 2, 2, 8, Z), F32),
        V((2, Y, Z), F32), V((ITERS, nx, Y, Z), F32), V((Y, Z), F32), V((Y, Z), F32),
        V((ITERS, 8, Z), F32), V((ITERS, nx * ny, Z), F32),
        dma((7,)), dma((4, 2)), dma((4, 2)), dma((4, 2, 2)), dma((4, 2, 2)),
        dma((4, 2, 2)), dma((4, 2, 2)), dma((ITERS, nx)), dma((ITERS, nx)),
        dma((ITERS,)), dma((ITERS,)),
    ]
    inside = pl.BlockSpec(memory_space=pltpu.VMEM)
    state = pl.pallas_call(
        functools.partial(kernel, nx, ny),
        out_shape=(pltpu.VMEM(padded, F32), pltpu.VMEM(padded, F32))
        + (pltpu.VMEM(cube, F32),) * 4 + (pltpu.VMEM((8, Z), F32),),
        in_specs=[pl.BlockSpec(memory_space=pltpu.HBM)] * 7,
        out_specs=(inside,) * 7,
        scratch_shapes=scratch,
        compiler_params=pltpu.CompilerParams(
            collective_id=0, has_side_effects=True, vmem_limit_bytes=48 * 1024 * 1024),
        name="inversion",
    )(zone_low, zone_high, density, slowness, pressure_obs, time_obs, zone_map)
    return pl.pallas_call(
        finish,
        out_shape=(
            jax.ShapeDtypeStruct(cube, F32),
            jax.ShapeDtypeStruct(cube, F32),
            jax.ShapeDtypeStruct((ITERS,), F32),
        ),
        in_specs=[inside] * 7,
        out_specs=(anyspace,) * 3,
        scratch_shapes=[V(cube, F32), V(cube, F32), pltpu.SMEM((ITERS,), F32), dma((9,))],
        compiler_params=pltpu.CompilerParams(vmem_limit_bytes=20 * 1024 * 1024),
        name="finish",
    )(*(pltpu.with_memory_space_constraint(a, pltpu.VMEM) for a in state))


def solution(mesh):
    cube = P("gx", "gy", None)
    return jax.shard_map(
        local,
        mesh=mesh,
        in_specs=(cube,) * 5 + (P(), P()),
        out_specs=(cube, cube, P()),
        check_vma=False,
    )
```

```python
import functools
import math

import jax
import jax.numpy as jnp
from jax import lax
from jax.experimental import pallas as pl
from jax.experimental.pallas import tpu as pltpu
from jax.sharding import PartitionSpec as P

ITERS = 3
BETA = 1.0
ETA = 0.5
EPSILON = 1e-06
MESH = pl.DeviceIdType.MESH
F32 = jnp.float32
BF16 = jnp.bfloat16
BOUNDS = 3
BANK = (0, 1, 0, 2)
UNROLL2 = 2
scope = jax.named_scope


def split(v):
    hi = v.astype(BF16)
    lo = (v - hi.astype(F32)).astype(BF16)
    return jnp.concatenate([hi, lo], axis=-1)


def kernel(
    nx, ny,
    zlow_h, zhigh_h, rho_h, sig_h, p_h, t_h, zone_h,
    both, grad, lim, stat,
    zlow, zhigh, p, t, zone, gp, lin,
    u1, v1, u2, v2, e3, f3, da, db, dedge, wts, ltab,
    rim, rim2, ysend, yrecv, xrecv, csend, crecv, pwsend, pwrecv, before, zsum, nsend, nrecv,
    insem, ys, yr, xs_, xr, cs, cr, ps, pr, ns, nr,
):
    X, Y, Z = p.shape
    rho, sig = both.at[0], both.at[1]
    grho, gsig = grad.at[0], grad.at[1]
    low, high = lim.at[0], lim.at[1]
    mx, my = lax.axis_index("gx"), lax.axis_index("gy")
    n = nx * ny
    N = nx * X
    cells = float(N * ny * Y * Z)
    zscale = 1.0 / math.sqrt(Z)
    xscale = 1.0 / math.sqrt(N)
    R = pl.ds(8, Y)
    XI = pl.ds(8, X)
    i0 = (mx * X).astype(F32)

    inner = (pl.ds(2, X), R)
    loads = [
        pltpu.make_async_copy(sig_h, sig.at[inner], insem.at[0]),
        pltpu.make_async_copy(rho_h, rho.at[inner], insem.at[1]),
        pltpu.make_async_copy(t_h, t, insem.at[2]),
        pltpu.make_async_copy(zone_h, zone, insem.at[3]),
        pltpu.make_async_copy(p_h, p, insem.at[4]),
        pltpu.make_async_copy(zlow_h, zlow, insem.at[5]),
        pltpu.make_async_copy(zhigh_h, zhigh, insem.at[6]),
    ]
    for c in loads:
        c.start()
    barrier = pltpu.get_barrier_semaphore()

    has = {0: (mx > 0, my > 0), 1: (mx < nx - 1, my < ny - 1)}
    sides = [(sx, sy) for sx in range(2) for sy in range(2)]

    def other(dx, dy):
        tx = lax.rem(mx + dx, nx) if dx else mx
        ty = lax.rem(my + dy, ny) if dy else my
        return tx, ty

    pairs = [(dx, dy) for dx in range(nx) for dy in range(ny)][1:]
    for dx, dy in pairs:
        pl.semaphore_signal(barrier, inc=1, device_id=other(dx, dy), device_id_type=MESH)

    for s in range(2):
        @pl.when(jnp.logical_not(has[s][1]))
        def _():
            for r in range(4):
                yrecv[r, s] = jnp.zeros(yrecv.shape[2:], F32)

        @pl.when(jnp.logical_not(has[s][0]))
        def _():
            for r in range(4):
                xrecv[r, s] = jnp.zeros(xrecv.shape[2:], F32)
    for sx, sy in sides:
        @pl.when(jnp.logical_not(jnp.logical_and(has[sx][0], has[sy][1])))
        def _():
            for r in range(4):
                crecv[r, sx, sy] = jnp.zeros((8, Z), F32)

    def ycopy(r, s):
        b = 1 if r == BOUNDS else 0
        return pltpu.make_async_remote_copy(
            src_ref=ysend.at[b, s], dst_ref=yrecv.at[r, 1 - s],
            send_sem=ys.at[s], recv_sem=yr.at[BANK[r], 1 - s],
            device_id=(mx, my + (2 * s - 1)), device_id_type=MESH)

    def xcopy(r, s):
        if r == 0:
            src = both.at[:, pl.ds(2 + s * (X - 2), 2), R]
        else:
            src = (lim if r == BOUNDS else grad).at[:, pl.ds(s * (X - 2), 2)]
        return pltpu.make_async_remote_copy(
            src_ref=src, dst_ref=xrecv.at[r, 1 - s],
            send_sem=xs_.at[s], recv_sem=xr.at[BANK[r], 1 - s],
            device_id=(mx + (2 * s - 1), my), device_id_type=MESH)

    def ccopy(r, sx, sy):
        b = 1 if r == BOUNDS else 0
        return pltpu.make_async_remote_copy(
            src_ref=csend.at[b, sx, sy, pl.ds(0, 2)], dst_ref=crecv.at[r, 1 - sx, 1 - sy, pl.ds(0, 2)],
            send_sem=cs.at[sx, sy], recv_sem=cr.at[BANK[r], 1 - sx, 1 - sy],
            device_id=(mx + (2 * sx - 1), my + (2 * sy - 1)), device_id_type=MESH)

    def rims_start(r):
        for sx, sy in sides:
            @pl.when(jnp.logical_and(has[sx][0], has[sy][1]))
            def _():
                ccopy(r, sx, sy).start()
        for s in range(2):
            @pl.when(has[s][1])
            def _():
                ycopy(r, s).start()

            @pl.when(has[s][0])
            def _():
                xcopy(r, s).start()

    def yrims_wait(r):
        for s in range(2):
            @pl.when(has[s][1])
            def _():
                ycopy(r, 1 - s).wait_recv()
        for sx, sy in sides:
            @pl.when(jnp.logical_and(has[sx][0], has[sy][1]))
            def _():
                ccopy(r, 1 - sx, 1 - sy).wait_recv()

    def xrims_wait(r):
        for s in range(2):
            @pl.when(has[s][0])
            def _():
                xcopy(r, 1 - s).wait_recv()

    def rims_sent(r):
        for s in range(2):
            @pl.when(has[s][1])
            def _():
                ycopy(r, s).wait_send()

            @pl.when(has[s][0])
            def _():
                xcopy(r, s).wait_send()
        for sx, sy in sides:
            @pl.when(jnp.logical_and(has[sx][0], has[sy][1]))
            def _():
                ccopy(r, sx, sy).wait_send()

    def pw_start(r):
        for dx in range(1, nx):
            tx, _ = other(dx, 0)
            pltpu.make_async_remote_copy(
                src_ref=pwsend.at[jnp.where(tx > mx, 0, 1)], dst_ref=pwrecv.at[r, dx - 1],
                send_sem=ps.at[0], recv_sem=pr.at[r % 2],
                device_id=(tx, my), device_id_type=MESH).start()

    def pw_wait(r):
        slots = pwrecv.at[r, pl.ds(0, nx - 1)]
        every = pltpu.make_async_remote_copy(
            src_ref=slots, dst_ref=slots, send_sem=ps.at[0], recv_sem=pr.at[r % 2],
            device_id=other(1, 0), device_id_type=MESH)
        every.wait_recv()
        every.wait_send()
        a = jnp.zeros((Y, Z), F32)
        b = jnp.zeros((Y, Z), F32)
        for dx in range(1, nx):
            w = jnp.where(dx <= mx, 1.0, 0.0)
            v = pwrecv[r, dx - 1]
            a = a + v * w
            b = b + v * (1.0 - w)
        return a, b

    def n_start(r):
        for d, (dx, dy) in enumerate(pairs):
            pltpu.make_async_remote_copy(
                src_ref=nsend.at[r, pl.ds(0, 1)], dst_ref=nrecv.at[r, pl.ds(d, 1)],
                send_sem=ns.at[0], recv_sem=nr.at[r % 2],
                device_id=other(dx, dy), device_id_type=MESH).start()

    def n_wait(r):
        rows = nrecv.at[r, pl.ds(0, n - 1)]
        every = pltpu.make_async_remote_copy(
            src_ref=rows, dst_ref=rows, send_sem=ns.at[0], recv_sem=nr.at[r % 2],
            device_id=other(0, 1), device_id_type=MESH)
        every.wait_recv()
        every.wait_send()
        return jnp.sum(nrecv[r], axis=0, keepdims=True)

    def fold(v):
        out = v[0:8]
        for k in range(8, v.shape[0], 8):
            out = out + v[k:k + 8]
        return out

    def gather(b, f, x, v):
        row = pl.ds(x, 1)
        ysend[b, 0, f, 0, row, :] = v[0:1]
        ysend[b, 0, f, 1, row, :] = v[1:2]
        ysend[b, 1, f, 0, row, :] = v[Y - 1:Y]
        ysend[b, 1, f, 1, row, :] = v[Y - 2:Y - 1]

    def corners(b):
        for f in range(2):
            for sx, sy in sides:
                csend[b, sx, sy, f:f + 1, :] = ysend[b, sy, f, 0, sx * (X - 1):sx * (X - 1) + 1, :]

    def slope(v):
        lane = lax.broadcasted_iota(jnp.int32, v.shape, 1)
        up = jnp.where(lane < Z - 1, pltpu.roll(v, Z - 1, 1), 0.0)
        return up - jnp.where(lane > 0, pltpu.roll(v, 1, 1), 0.0)

    zero = jnp.zeros((Y, Z), F32)
    z8 = jnp.zeros((8, Z), F32)

    with scope("load02"):
        loads[0].wait()
        loads[2].wait()

    def sums(x, carry):
        a, b, c = carry
        v = sig[x + 2, R, :]
        gather(0, 1, x, v)
        weight = float(N) - i0 - x.astype(F32)
        return a + v, b + weight * v, c + t[x]

    psum_, wsum, tsum = lax.fori_loop(0, X, sums, (zero, zero, zero), unroll=4)
    zown = xscale * wsum - tsum
    pwsend[0] = psum_
    pwsend[1] = zown
    loads[1].wait()

    def copy_rho(x, carry):
        gather(0, 0, x, rho[x + 2, R, :])
        return carry

    lax.fori_loop(0, X, copy_rho, 0, unroll=4)
    corners(0)
    with scope("barrier"):
        pl.semaphore_wait(barrier, n - 1)
    with scope("rims0start"):
        rims_start(0)
        pw_start(0)

    for c in loads[3:]:
        c.wait()

    def bounds(x, carry):
        ids = zone[x]
        lo = jnp.zeros((Y, Z), F32)
        hi = jnp.zeros((Y, Z), F32)
        for k in range(zlow.shape[0]):
            hit = ids == k
            lo = jnp.where(hit, zlow[k], lo)
            hi = jnp.where(hit, zhigh[k], hi)
        low[x] = lo
        high[x] = hi
        gather(1, 0, x, lo)
        gather(1, 1, x, hi)
        return carry

    with scope("bounds"):
        lax.fori_loop(0, X, bounds, 0, unroll=2)
        corners(1)

    ri = lax.broadcasted_iota(jnp.int32, (Z, Z), 0)
    ci = lax.broadcasted_iota(jnp.int32, (Z, Z), 1)
    m = (Z - jnp.maximum(ri, ci)).astype(F32).astype(BF16)
    u = jnp.where(ri <= ci, 1.0, 0.0).astype(BF16)
    band = jnp.where(ri == ci + 1, 1.0, jnp.where(ri == ci - 1, -1.0, 0.0)).astype(BF16)
    l = jnp.where(ri >= ci, 1.0, 0.0).astype(BF16)
    for half in (slice(0, Z), slice(Z, 2 * Z)):
        wts[half, 0:Z] = m
        wts[half, Z:2 * Z] = band
        wts[half, 2 * Z:3 * Z] = u
        ltab[half] = l

    with scope("pback"):
        v = p[...].reshape(X * Y, Z)
        out = jnp.dot(split(v), ltab[...], preferred_element_type=F32)
        gp[...] = (out * zscale).reshape(X, Y, Z)

    def zslope(v):
        return jnp.dot(split(v), wts[:, Z:2 * Z], preferred_element_type=F32)

    def zlin():
        v = rho[inner[0], R, :].reshape(X * Y, Z)
        out = jnp.dot(split(v), wts[...], preferred_element_type=F32)
        lin[...] = out[:, 0:Z].reshape(X, Y, Z)
        da[...] = out[:, Z:2 * Z].reshape(X, Y, Z)
        rp = zscale * out[:, 2 * Z:3 * Z].reshape(X, Y, Z) - p[...]
        v = sig[inner[0], R, :].reshape(X * Y, Z)
        db[...] = zslope(v).reshape(X, Y, Z)
        return fold((rp * rp).reshape(X * Y, Z))

    def edges():
        dedge[...] = slope(jnp.concatenate(
            [rim[f, s, 1, XI, :] for f in range(2) for s in range(2)], axis=0))

    def set_rows(x, carry):
        for f, a in ((0, rho), (1, sig)):
            for s in range(2):
                a[x + 2, pl.ds(7 + s * (Y + 1), 1), :] = rim[f, s, 1, pl.ds(8 + x, 1), :]
        return carry

    def set_corners():
        for f, a in ((0, rho), (1, sig)):
            for sx, sy in sides:
                a[1 + sx * (X + 1), pl.ds(7 + sy * (Y + 1), 1), :] = (
                    rim[f, sy, 1, 7 + sx * (X + 1):8 + sx * (X + 1), :])

    for k in range(ITERS):
        if k > 0:
            def update(i, carry):
                rho[i + 2, R, :] = jnp.minimum(jnp.maximum(rho[i + 2, R, :] - step_r * grho[i], low[i]), high[i])
                sig[i + 2, R, :] = sig[i + 2, R, :] - step_s * gsig[i]
                return carry

            with scope("update"):
                lax.fori_loop(0, X, update, 0, unroll=4)
        with scope("zlin"):
            psq = zlin()
        if k == 0:
            with scope("yrimwait"):
                yrims_wait(0)
            for f, a in ((0, rho), (1, sig)):
                for s in range(2):
                    rim[f, s, 0, XI, :] = yrecv[0, s, f, 1]
                    rim[f, s, 1, XI, :] = yrecv[0, s, f, 0]
                    rim[f, s, 2, XI, :] = ysend[0, s, f, 0]
                    for sx in range(2):
                        rim[f, s, 1, 7 + sx * (X + 1):8 + sx * (X + 1), :] = crecv[0, sx, s, f:f + 1, :]
        else:
            with scope("yrimwait"):
                if k == 1:
                    yrims_wait(BOUNDS)
                yrims_wait(k)
            for s in range(2):
                for row, slot in ((0, 1), (1, 0), (2, 0)):
                    gr = (ysend[0, s, 0, 0] if row == 2 else yrecv[k, s, 0, slot])
                    gs = (ysend[0, s, 1, 0] if row == 2 else yrecv[k, s, 1, slot])
                    lo = (ysend[1, s, 0, 0] if row == 2 else yrecv[3, s, 0, slot])
                    hi = (ysend[1, s, 1, 0] if row == 2 else yrecv[3, s, 1, slot])
                    rim[0, s, row, XI, :] = jnp.minimum(jnp.maximum(rim[0, s, row, XI, :] - step_r * gr, lo), hi)
                    rim[1, s, row, XI, :] = rim[1, s, row, XI, :] - step_s * gs
                for sx in range(2):
                    at = slice(7 + sx * (X + 1), 8 + sx * (X + 1))
                    rim[0, s, 1, at, :] = jnp.minimum(jnp.maximum(
                        rim[0, s, 1, at, :] - step_r * crecv[k, sx, s, 0:1, :],
                        crecv[3, sx, s, 0:1, :]), crecv[3, sx, s, 1:2, :])
                    rim[1, s, 1, at, :] = rim[1, s, 1, at, :] - step_s * crecv[k, sx, s, 1:2, :]
        with scope("setrows"):
            lax.fori_loop(0, X, set_rows, 0, unroll=4)
            set_corners()
        with scope("edges"):
            edges()

        for s in range(2):
            def rimstep(q, carry):
                base = pl.multiple_of(q * 8, 8)
                def vec(f):
                    a1 = rim[f, s, 1, pl.ds(9 + base, 8), :] - rim[f, s, 1, pl.ds(7 + base, 8), :]
                    a2 = rim[f, s, 2 - 2 * s, pl.ds(8 + base, 8), :] - rim[f, s, 2 * s, pl.ds(8 + base, 8), :]
                    return a1, a2, dedge[pl.ds((2 * f + s) * X + base, 8), :]
                a1, a2, a3 = vec(0)
                b1, b2, b3 = vec(1)
                c1 = a2 * b3 - a3 * b2
                c3 = a1 * b2 - a2 * b1
                rim2[s, 0, pl.ds(base, 8), :] = b3 * c1 - b1 * c3
                rim2[s, 1, pl.ds(base, 8), :] = c3 * a1 - c1 * a3
                return carry
            with scope("rimstep"):
                lax.fori_loop(0, X // 8, rimstep, 0)

        def vectors(a, x, a3):
            a1 = a[x + 1, R, :] - a[x - 1, R, :]
            a2 = a[x, pl.ds(9, Y), :] - a[x, pl.ds(7, Y), :]
            return a1, a2, a3

        def edge(x):
            a1, a2, a3 = vectors(rho, x, slope(rho[x, R, :]))
            b1, b2, b3 = vectors(sig, x, slope(sig[x, R, :]))
            c2 = a3 * b1 - a1 * b3
            c3 = a1 * b2 - a2 * b1
            u1[x - 1] = b2 * c3 - b3 * c2
            v1[x - 1] = c2 * a3 - c3 * a2

        def pass1(i, acc):
            x = i + 2
            a1, a2, a3 = vectors(rho, x, da[i])
            b1, b2, b3 = vectors(sig, x, db[i])
            c1 = a2 * b3 - a3 * b2
            c2 = a3 * b1 - a1 * b3
            c3 = a1 * b2 - a2 * b1
            u1[i + 1] = b2 * c3 - b3 * c2
            v1[i + 1] = c2 * a3 - c3 * a2
            u2[i, R, :] = b3 * c1 - b1 * c3
            v2[i, R, :] = c3 * a1 - c1 * a3
            e3[i] = b1 * c2 - b2 * c1
            f3[i] = c1 * a2 - c2 * a1
            for s in range(2):
                at = pl.ds(7 + s * (Y + 1), 1)
                u2[i, at, :] = rim2[s, 0, pl.ds(i, 1), :]
                v2[i, at, :] = rim2[s, 1, pl.ds(i, 1), :]
            return acc + fold(c1 * c1 + c2 * c2 + c3 * c3)

        with scope("pass1"):
            csq = lax.fori_loop(2, X - 2, pass1, z8, unroll=4)
            csq = pass1(1, csq)
            csq = pass1(X - 2, csq)
        with scope("xrimwait"):
            if k == 1:
                xrims_wait(BOUNDS)
            xrims_wait(k)
        for s in range(2):
            pls = pl.ds(s * (X + 2), 2)
            if k == 0:
                rho[pls, R, :] = xrecv[0, s, 0]
                sig[pls, R, :] = xrecv[0, s, 1]
            else:
                rho[pls, R, :] = jnp.minimum(jnp.maximum(
                    rho[pls, R, :] - step_r * xrecv[k, s, 0], xrecv[3, s, 0]), xrecv[3, s, 1])
                sig[pls, R, :] = sig[pls, R, :] - step_s * xrecv[k, s, 1]
        rims_sent(k)
        if k == 0:
            with scope("rims3start"):
                rims_start(BOUNDS)
        with scope("edge"):
            edge(1)
            edge(X + 2)
            csq = pass1(0, csq)
            csq = pass1(X - 1, csq)

        with scope("pwwait"):
            if k == 0:
                a, b = pw_wait(0)
                before[...] = a
                zsum[...] = b + zown
            else:
                a, b = pw_wait(k)
                before[...] = before[...] - step_s * a
                zsum[...] = zsum[...] - (step_s * xscale) * (b + wg)
        start = xscale * (float(N) - i0) * before[...] + zsum[...]

        def pass2(i, carry):
            pref, back, acc, nrho, nsig = carry
            v = sig[i + 2, R, :]
            pref = pref + v
            rt = xscale * pref - t[i]
            adj_s = (v1[i] - v1[i + 2]) + (v2[i, pl.ds(7, Y), :] - v2[i, pl.ds(9, Y), :]) - f3[i]
            gs = xscale * back + (BETA / 16.0) * adj_s
            back = back - rt
            adj_r = (u1[i] - u1[i + 2]) + (u2[i, pl.ds(7, Y), :] - u2[i, pl.ds(9, Y), :]) - e3[i]
            gr = (zscale * zscale) * lin[i] - gp[i] + (BETA / 16.0) * adj_r
            grho[i] = gr
            gsig[i] = gs
            acc = acc + fold(rt * rt)
            nrho = nrho + fold(gr * gr)
            nsig = nsig + fold(gs * gs)
            if k < ITERS - 1:
                gather(0, 0, i, gr)
                gather(0, 1, i, gs)
            return pref, back, acc, nrho, nsig

        with scope("zadj"):
            for a in (e3, f3):
                a[...] = zslope(a[...].reshape(X * Y, Z)).reshape(X, Y, Z)
        with scope("pass2"):
            _, _, acc, nrho, nsig = lax.fori_loop(
                0, X, pass2, (before[...], start, z8, z8, z8), unroll=UNROLL2)
        local = (0.5 / cells) * (acc + psq + (BETA / 16.0) * csq)
        lane = lax.broadcasted_iota(jnp.int32, (1, Z), 1)

        def total(v):
            return jnp.sum(jnp.sum(v, axis=0, keepdims=True), axis=1, keepdims=True)

        row = jnp.where(lane < 1, total(nrho), jnp.where(lane < 2, total(nsig), total(local)))
        nsend[k, 0:1] = row
        nrecv[k, n - 1:n] = row
        with scope("nstart"):
            n_start(k)
        if k < ITERS - 1:
            with scope("rimstart"):
                corners(0)
                if k == 0:
                    rims_sent(BOUNDS)
                rims_start(k + 1)

            def weigh(i, carry):
                pg, wg = carry
                gs = gsig[i]
                return pg + gs, wg + (float(N) - i0 - i.astype(F32)) * gs

            with scope("weigh"):
                pg, wg = lax.fori_loop(0, X, weigh, (zero, zero), unroll=8)
                pwsend[0] = pg
                pwsend[1] = wg
                pw_start(k + 1)
        with scope("nwait"):
            tot = n_wait(k)
        steps = ETA * lax.rsqrt(tot / cells + EPSILON)
        step_r = jnp.broadcast_to(steps[0:1, 0:1], (1, Z))
        step_s = jnp.broadcast_to(steps[0:1, 1:2], (1, Z))
        stat[k:k + 1, :] = jnp.broadcast_to(tot[0:1, 2:3], (1, Z))
        if k == ITERS - 1:
            stat[ITERS:ITERS + 1, :] = step_r
            stat[ITERS + 1:ITERS + 2, :] = step_s


def finish(both, grad, lim, stat, rho_o, sig_o, obj_o, rho_b, sig_b, obj, sems):
    X, Y, Z = rho_b.shape
    R = pl.ds(8, Y)
    seen = stat[...]
    for k in range(ITERS):
        obj[k] = seen[k, 0]
    copies = [pltpu.make_async_copy(obj, obj_o, sems.at[0])]
    copies[0].start()
    step_r = stat[ITERS:ITERS + 1, :]
    step_s = stat[ITERS + 1:ITERS + 2, :]

    def move(i, carry):
        rho_b[i] = jnp.minimum(jnp.maximum(both[0, i + 2, R, :] - step_r * grad[0, i], lim[0, i]), lim[1, i])
        sig_b[i] = both[1, i + 2, R, :] - step_s * grad[1, i]
        return carry

    parts = 4
    for c in range(parts):
        lax.fori_loop(c * X // parts, (c + 1) * X // parts, move, 0, unroll=4)
        rows = pl.ds(c * X // parts, X // parts)
        for f, (a, b) in enumerate(((rho_b, rho_o), (sig_b, sig_o))):
            copies.append(pltpu.make_async_copy(a.at[rows], b.at[rows], sems.at[1 + 2 * c + f]))
            copies[-1].start()
    for c in copies:
        c.wait()


def local(density, slowness, pressure_obs, time_obs, zone_map, zone_low, zone_high):
    X, Y, Z = density.shape
    nx, ny = lax.axis_size("gx"), lax.axis_size("gy")
    assert Z <= 256
    V = pltpu.VMEM
    cube = (X, Y, Z)
    padded = (2, X + 4, Y + 16, Z)
    dma = pltpu.SemaphoreType.DMA
    anyspace = pl.BlockSpec(memory_space=pl.ANY)
    zones = zone_low.shape[0]
    scratch = [
        pltpu.SMEM((zones,), F32), pltpu.SMEM((zones,), F32),
        V(cube, F32), V(cube, F32),
        V(cube, jnp.int32), V(cube, F32), V(cube, F32),
        V((X + 2, Y, Z), F32), V((X + 2, Y, Z), F32), V((X, Y + 16, Z), F32), V((X, Y + 16, Z), F32),
        V(cube, F32), V(cube, F32), V(cube, F32), V(cube, F32), V((4 * X, Z), F32),
        V((2 * Z, 3 * Z), BF16), V((2 * Z, Z), BF16),
        V((2, 2, 3, X + 16, Z), F32), V((2, 2, X, Z), F32),
        V((2, 2, 2, 2, X, Z), F32), V((4, 2, 2, 2, X, Z), F32), V((4, 2, 2, 2, Y, Z), F32),
        V((2, 2, 2, 8, Z), F32), V((4, 2, 2, 8, Z), F32),
        V((2, Y, Z), F32), V((ITERS, nx - 1, Y, Z), F32), V((Y, Z), F32), V((Y, Z), F32),
        V((ITERS, 8, Z), F32), V((ITERS, nx * ny, Z), F32),
        dma((7,)), dma((2,)), dma((3, 2)), dma((2,)), dma((3, 2)),
        dma((2, 2)), dma((3, 2, 2)), dma((1,)), dma((2,)),
        dma((1,)), dma((2,)),
    ]
    inside = pl.BlockSpec(memory_space=pltpu.VMEM)
    state = pl.pallas_call(
        functools.partial(kernel, nx, ny),
        out_shape=(V(padded, F32), V((2,) + cube, F32), V((2,) + cube, F32), V((8, Z), F32)),
        in_specs=[pl.BlockSpec(memory_space=pltpu.HBM)] * 7,
        out_specs=(inside,) * 4,
        scratch_shapes=scratch,
        compiler_params=pltpu.CompilerParams(
            collective_id=0, has_side_effects=True, vmem_limit_bytes=48 * 1024 * 1024),
        name="inversion",
    )(zone_low, zone_high, density, slowness, pressure_obs, time_obs, zone_map)
    return pl.pallas_call(
        finish,
        out_shape=(
            jax.ShapeDtypeStruct(cube, F32),
            jax.ShapeDtypeStruct(cube, F32),
            jax.ShapeDtypeStruct((ITERS,), F32),
        ),
        in_specs=[inside] * 4,
        out_specs=(anyspace,) * 3,
        scratch_shapes=[V(cube, F32), V(cube, F32), pltpu.SMEM((ITERS,), F32), dma((9,))],
        compiler_params=pltpu.CompilerParams(vmem_limit_bytes=20 * 1024 * 1024),
        name="finish",
    )(*(pltpu.with_memory_space_constraint(a, pltpu.VMEM) for a in state))


def solution(mesh):
    cube = P("gx", "gy", None)
    return jax.shard_map(
        local,
        mesh=mesh,
        in_specs=(cube,) * 5 + (P(), P()),
        out_specs=(cube, cube, P()),
        check_vma=False,
    )
```

```python
import functools
import math

import jax
import jax.numpy as jnp
from jax import lax
from jax.experimental import pallas as pl
from jax.experimental.pallas import tpu as pltpu
from jax.sharding import PartitionSpec as P

ITERS = 3
BETA = 1.0
ETA = 0.5
EPSILON = 1e-06
MESH = pl.DeviceIdType.MESH
F32 = jnp.float32
BF16 = jnp.bfloat16
BOUNDS = 3
BANK = (0, 1, 0, 2)
UNROLL2 = 2
GROUP = 8
scope = jax.named_scope


def split(v):
    hi = v.astype(BF16)
    lo = (v - hi.astype(F32)).astype(BF16)
    return jnp.concatenate([hi, lo], axis=-1)


def kernel(
    nx, ny,
    zlow_h, zhigh_h, rho_h, sig_h, p_h, t_h, zone_h,
    both, grad, lim, stat,
    zlow, zhigh, p, t, zone, gp, lin,
    u1, v1, u2, v2, e3, f3, da, db, dg, miss, c1s, c2s, c3s, dedge, wts, ltab,
    zsend, zyrecv, zxrecv, zcsend, zcrecv,
    rim, rim2, ysend, yrecv, xrecv, csend, crecv, pwsend, pwrecv, before, zsum, nsend, nrecv,
    insem, ys, yr, xs_, xr, cs, cr, ps, pr, ns, nr,
):
    X, Y, Z = p.shape
    rho, sig = both.at[0], both.at[1]
    grho, gsig = grad.at[0], grad.at[1]
    low, high = lim.at[0], lim.at[1]
    mx, my = lax.axis_index("gx"), lax.axis_index("gy")
    n = nx * ny
    N = nx * X
    cells = float(N * ny * Y * Z)
    zscale = 1.0 / math.sqrt(Z)
    xscale = 1.0 / math.sqrt(N)
    gain = 16.0 / BETA
    tscale = gain * xscale
    R = pl.ds(8, Y)
    XI = pl.ds(8, X)
    i0 = (mx * X).astype(F32)

    inner = (pl.ds(2, X), R)
    loads = [
        pltpu.make_async_copy(sig_h, sig.at[inner], insem.at[0]),
        pltpu.make_async_copy(rho_h, rho.at[inner], insem.at[1]),
        pltpu.make_async_copy(t_h, t, insem.at[2]),
        pltpu.make_async_copy(zone_h, zone, insem.at[3]),
        pltpu.make_async_copy(p_h, p, insem.at[4]),
        pltpu.make_async_copy(zlow_h, zlow, insem.at[5]),
        pltpu.make_async_copy(zhigh_h, zhigh, insem.at[6]),
    ]
    for c in loads:
        c.start()
    barrier = pltpu.get_barrier_semaphore()

    has = {0: (mx > 0, my > 0), 1: (mx < nx - 1, my < ny - 1)}
    sides = [(sx, sy) for sx in range(2) for sy in range(2)]

    def other(dx, dy):
        tx = lax.rem(mx + dx, nx) if dx else mx
        ty = lax.rem(my + dy, ny) if dy else my
        return tx, ty

    pairs = [(dx, dy) for dx in range(nx) for dy in range(ny)][1:]
    for dx, dy in pairs:
        pl.semaphore_signal(barrier, inc=1, device_id=other(dx, dy), device_id_type=MESH)

    def blank(ref, at, value):
        ref[at] = jnp.full(ref.shape[len(at):], value, ref.dtype)

    for s in range(2):
        @pl.when(jnp.logical_not(has[s][1]))
        def _():
            blank(zyrecv, (s,), -1)
            for r in range(ITERS):
                blank(yrecv, (r, s), 0.0)

        @pl.when(jnp.logical_not(has[s][0]))
        def _():
            blank(zxrecv, (s,), -1)
            for r in range(ITERS):
                blank(xrecv, (r, s), 0.0)
    for sx, sy in sides:
        @pl.when(jnp.logical_not(jnp.logical_and(has[sx][0], has[sy][1])))
        def _():
            blank(zcrecv, (sx, sy), -1)
            for r in range(ITERS):
                blank(crecv, (r, sx, sy), 0.0)

    def ycopy(r, s):
        b = 1 if r == BOUNDS else 0
        return pltpu.make_async_remote_copy(
            src_ref=zsend.at[s] if b else ysend.at[0, s],
            dst_ref=zyrecv.at[1 - s] if b else yrecv.at[r, 1 - s],
            send_sem=ys.at[b, s], recv_sem=yr.at[BANK[r], 1 - s],
            device_id=(mx, my + (2 * s - 1)), device_id_type=MESH)

    def xcopy(r, s):
        b = 1 if r == BOUNDS else 0
        planes = pl.ds(s * (X - 2), 2)
        if r == 0:
            src = both.at[:, pl.ds(2 + s * (X - 2), 2), R]
        else:
            src = zone.at[planes] if b else grad.at[:, planes]
        return pltpu.make_async_remote_copy(
            src_ref=src, dst_ref=zxrecv.at[1 - s] if b else xrecv.at[r, 1 - s],
            send_sem=xs_.at[b, s], recv_sem=xr.at[BANK[r], 1 - s],
            device_id=(mx + (2 * s - 1), my), device_id_type=MESH)

    def ccopy(r, sx, sy):
        b = 1 if r == BOUNDS else 0
        src = zcsend.at[sx, sy, pl.ds(0, 1)] if b else csend.at[sx, sy, pl.ds(0, 2)]
        dst = zcrecv.at[1 - sx, 1 - sy, pl.ds(0, 1)] if b else crecv.at[r, 1 - sx, 1 - sy, pl.ds(0, 2)]
        return pltpu.make_async_remote_copy(
            src_ref=src, dst_ref=dst,
            send_sem=cs.at[b, sx, sy], recv_sem=cr.at[BANK[r], 1 - sx, 1 - sy],
            device_id=(mx + (2 * sx - 1), my + (2 * sy - 1)), device_id_type=MESH)

    def rims_start(r):
        for sx, sy in sides:
            @pl.when(jnp.logical_and(has[sx][0], has[sy][1]))
            def _():
                ccopy(r, sx, sy).start()
        for s in range(2):
            @pl.when(has[s][1])
            def _():
                ycopy(r, s).start()

            @pl.when(has[s][0])
            def _():
                xcopy(r, s).start()

    def yrims_wait(r):
        for s in range(2):
            @pl.when(has[s][1])
            def _():
                ycopy(r, 1 - s).wait_recv()
        for sx, sy in sides:
            @pl.when(jnp.logical_and(has[sx][0], has[sy][1]))
            def _():
                ccopy(r, 1 - sx, 1 - sy).wait_recv()

    def xrims_wait(r):
        for s in range(2):
            @pl.when(has[s][0])
            def _():
                xcopy(r, 1 - s).wait_recv()

    def rims_sent(r):
        for s in range(2):
            @pl.when(has[s][1])
            def _():
                ycopy(r, s).wait_send()

            @pl.when(has[s][0])
            def _():
                xcopy(r, s).wait_send()
        for sx, sy in sides:
            @pl.when(jnp.logical_and(has[sx][0], has[sy][1]))
            def _():
                ccopy(r, sx, sy).wait_send()

    def pw_start(r):
        for dx in range(1, nx):
            tx, _ = other(dx, 0)
            pltpu.make_async_remote_copy(
                src_ref=pwsend.at[jnp.where(tx > mx, 0, 1)], dst_ref=pwrecv.at[r, dx - 1],
                send_sem=ps.at[0], recv_sem=pr.at[r % 2],
                device_id=(tx, my), device_id_type=MESH).start()

    def pw_wait(r):
        slots = pwrecv.at[r, pl.ds(0, nx - 1)]
        every = pltpu.make_async_remote_copy(
            src_ref=slots, dst_ref=slots, send_sem=ps.at[0], recv_sem=pr.at[r % 2],
            device_id=other(1, 0), device_id_type=MESH)
        every.wait_recv()
        every.wait_send()
        a = jnp.zeros((Y, Z), F32)
        b = jnp.zeros((Y, Z), F32)
        for dx in range(1, nx):
            w = jnp.where(dx <= mx, 1.0, 0.0)
            v = pwrecv[r, dx - 1]
            a = a + v * w
            b = b + v * (1.0 - w)
        return a, b

    def n_start(r):
        for d, (dx, dy) in enumerate(pairs):
            pltpu.make_async_remote_copy(
                src_ref=nsend.at[r, pl.ds(0, 1)], dst_ref=nrecv.at[r, pl.ds(d, 1)],
                send_sem=ns.at[0], recv_sem=nr.at[r % 2],
                device_id=other(dx, dy), device_id_type=MESH).start()

    def n_wait(r):
        rows = nrecv.at[r, pl.ds(0, n - 1)]
        every = pltpu.make_async_remote_copy(
            src_ref=rows, dst_ref=rows, send_sem=ns.at[0], recv_sem=nr.at[r % 2],
            device_id=other(0, 1), device_id_type=MESH)
        every.wait_recv()
        every.wait_send()
        return jnp.sum(nrecv[r], axis=0, keepdims=True)

    def fold(v):
        out = v[0:8]
        for k in range(8, v.shape[0], 8):
            out = out + v[k:k + 8]
        return out

    def gather(b, f, x, v):
        row = pl.ds(x, 1)
        ysend[b, 0, f, 0, row, :] = v[0:1]
        ysend[b, 0, f, 1, row, :] = v[1:2]
        ysend[b, 1, f, 0, row, :] = v[Y - 1:Y]
        ysend[b, 1, f, 1, row, :] = v[Y - 2:Y - 1]

    def corners():
        for f in range(2):
            for sx, sy in sides:
                csend[sx, sy, f:f + 1, :] = ysend[0, sy, f, 0, sx * (X - 1):sx * (X - 1) + 1, :]

    def slope(v):
        lane = lax.broadcasted_iota(jnp.int32, v.shape, 1)
        up = jnp.where(lane < Z - 1, pltpu.roll(v, Z - 1, 1), 0.0)
        return up - jnp.where(lane > 0, pltpu.roll(v, 1, 1), 0.0)

    zero = jnp.zeros((Y, Z), F32)
    z8 = jnp.zeros((8, Z), F32)

    with scope("load02"):
        loads[0].wait()
        loads[2].wait()

    def sums(x, carry):
        a, b, c = carry
        v = sig[x + 2, R, :]
        gather(0, 1, x, v)
        weight = float(N) - i0 - x.astype(F32)
        return a + v, b + weight * v, c + t[x]

    psum_, wsum, tsum = lax.fori_loop(0, X, sums, (zero, zero, zero), unroll=4)
    zown = xscale * wsum - tsum
    pwsend[0] = psum_
    pwsend[1] = zown
    loads[1].wait()

    def copy_rho(x, carry):
        gather(0, 0, x, rho[x + 2, R, :])
        return carry

    lax.fori_loop(0, X, copy_rho, 0, unroll=4)
    corners()
    with scope("barrier"):
        pl.semaphore_wait(barrier, n - 1)
    with scope("rims0start"):
        rims_start(0)
        pw_start(0)

    for c in loads[3:]:
        c.wait()

    def limits(ids):
        lo = jnp.zeros(ids.shape, F32)
        hi = jnp.zeros(ids.shape, F32)
        for k in range(zlow.shape[0]):
            hit = ids == k
            lo = jnp.where(hit, zlow[k], lo)
            hi = jnp.where(hit, zhigh[k], hi)
        return lo, hi

    def bounds(x, carry):
        ids = zone[x]
        lo, hi = limits(ids)
        row = pl.ds(x, 1)
        for s in range(2):
            for slot in range(2):
                at = s * (Y - 1) + (1 - 2 * s) * slot
                zsend[s, slot, row, :] = ids[at:at + 1]
        low[x] = lo
        high[x] = hi
        t[x] = tscale * t[x]
        gather(1, 0, x, lo)
        gather(1, 1, x, hi)
        return carry

    with scope("bounds"):
        lax.fori_loop(0, X, bounds, 0, unroll=2)
        for sx, sy in sides:
            zcsend[sx, sy, 0:1, :] = zsend[sy, 0, sx * (X - 1):sx * (X - 1) + 1, :]

    ri = lax.broadcasted_iota(jnp.int32, (Z, Z), 0)
    ci = lax.broadcasted_iota(jnp.int32, (Z, Z), 1)
    m = (Z - jnp.maximum(ri, ci)).astype(F32).astype(BF16)
    u = jnp.where(ri <= ci, 1.0, 0.0).astype(BF16)
    band = jnp.where(ri == ci + 1, 1.0, jnp.where(ri == ci - 1, -1.0, 0.0)).astype(BF16)
    l = jnp.where(ri >= ci, 1.0, 0.0).astype(BF16)
    for half in (slice(0, Z), slice(Z, 2 * Z)):
        wts[half, 0:Z] = m
        wts[half, Z:2 * Z] = band
        wts[half, 2 * Z:3 * Z] = u
        ltab[half] = l

    with scope("pback"):
        v = p[...].reshape(X * Y, Z)
        out = jnp.dot(split(v), ltab[...], preferred_element_type=F32)
        gp[...] = (out * (gain * zscale)).reshape(X, Y, Z)

    def product(v, columns):
        rows = v.shape[0] // 2
        return jnp.concatenate([
            jnp.dot(split(v[h * rows:(h + 1) * rows]), wts[:, columns], preferred_element_type=F32)
            for h in range(2)], axis=0)

    def zslope(v):
        return product(v, slice(Z, 2 * Z))

    def zlin(v, columns):
        out = product(v.reshape(X * Y, Z), slice(0, columns * Z))
        lin[...] = (out[:, 0:Z] * (gain * zscale * zscale)).reshape(X, Y, Z)
        da[...] = out[:, Z:2 * Z].reshape(X, Y, Z)
        return pressure(out[:, 2 * Z:3 * Z]) if columns > 2 else None

    def pressure(v):
        rp = zscale * v - p[...].reshape(X * Y, Z)
        return fold(rp * rp)

    def edges():
        dedge[...] = slope(jnp.concatenate(
            [rim[f, s, 1, XI, :] for f in range(2) for s in range(2)], axis=0))

    def set_rows(x, carry):
        for f, a in ((0, rho), (1, sig)):
            for s in range(2):
                a[x + 2, pl.ds(7 + s * (Y + 1), 1), :] = rim[f, s, 1, pl.ds(8 + x, 1), :]
        return carry

    def set_corners():
        for f, a in ((0, rho), (1, sig)):
            for sx, sy in sides:
                a[1 + sx * (X + 1), pl.ds(7 + sy * (Y + 1), 1), :] = (
                    rim[f, sy, 1, 7 + sx * (X + 1):8 + sx * (X + 1), :])

    for k in range(ITERS):
        late = k == ITERS - 1
        if k == 0:
            with scope("zlin"):
                psq = zlin(rho[inner[0], R, :], 3)
                db[...] = zslope(sig[inner[0], R, :].reshape(X * Y, Z)).reshape(X, Y, Z)
        else:
            with scope("update"):
                v = jnp.minimum(jnp.maximum(rho[inner[0], R, :] - step_r * grho[...], low[...]), high[...])
                rho[inner[0], R, :] = v
                sig[inner[0], R, :] = sig[inner[0], R, :] - step_s * gsig[...]
                db[...] = db[...] - step_s * dg[...]
                psq = zlin(v, 3 if late else 2)
        if k == 0:
            with scope("yrimwait"):
                yrims_wait(0)
            with scope("rims3start"):
                rims_start(BOUNDS)
            for f, a in ((0, rho), (1, sig)):
                for s in range(2):
                    rim[f, s, 0, XI, :] = yrecv[0, s, f, 1]
                    rim[f, s, 1, XI, :] = yrecv[0, s, f, 0]
                    rim[f, s, 2, XI, :] = ysend[0, s, f, 0]
                    for sx in range(2):
                        rim[f, s, 1, 7 + sx * (X + 1):8 + sx * (X + 1), :] = crecv[0, sx, s, f:f + 1, :]
        else:
            with scope("yrimwait"):
                yrims_wait(k)
            for s in range(2):
                for row, slot in ((0, 1), (1, 0), (2, 0)):
                    gr = (ysend[0, s, 0, 0] if row == 2 else yrecv[k, s, 0, slot])
                    gs = (ysend[0, s, 1, 0] if row == 2 else yrecv[k, s, 1, slot])
                    lo = (ysend[1, s, 0, 0] if row == 2 else yrecv[3, s, 0, slot])
                    hi = (ysend[1, s, 1, 0] if row == 2 else yrecv[3, s, 1, slot])
                    rim[0, s, row, XI, :] = jnp.minimum(jnp.maximum(rim[0, s, row, XI, :] - step_r * gr, lo), hi)
                    rim[1, s, row, XI, :] = rim[1, s, row, XI, :] - step_s * gs
                for sx in range(2):
                    at = slice(7 + sx * (X + 1), 8 + sx * (X + 1))
                    rim[0, s, 1, at, :] = jnp.minimum(jnp.maximum(
                        rim[0, s, 1, at, :] - step_r * crecv[k, sx, s, 0:1, :],
                        crecv[3, sx, s, 0:1, :]), crecv[3, sx, s, 1:2, :])
                    rim[1, s, 1, at, :] = rim[1, s, 1, at, :] - step_s * crecv[k, sx, s, 1:2, :]
        with scope("setrows"):
            lax.fori_loop(0, X, set_rows, 0, unroll=4)
            set_corners()
        with scope("edges"):
            edges()

        for s in range(2):
            def rimstep(q, carry):
                base = pl.multiple_of(q * 8, 8)
                def vec(f):
                    a1 = rim[f, s, 1, pl.ds(9 + base, 8), :] - rim[f, s, 1, pl.ds(7 + base, 8), :]
                    a2 = rim[f, s, 2 - 2 * s, pl.ds(8 + base, 8), :] - rim[f, s, 2 * s, pl.ds(8 + base, 8), :]
                    return a1, a2, dedge[pl.ds((2 * f + s) * X + base, 8), :]
                a1, a2, a3 = vec(0)
                b1, b2, b3 = vec(1)
                c1 = a2 * b3 - a3 * b2
                c3 = a1 * b2 - a2 * b1
                rim2[s, 0, pl.ds(base, 8), :] = b3 * c1 - b1 * c3
                rim2[s, 1, pl.ds(base, 8), :] = c3 * a1 - c1 * a3
                return carry
            with scope("rimstep"):
                lax.fori_loop(0, X // 8, rimstep, 0)

        def vectors(a, x, a3):
            a1 = a[x + 1, R, :] - a[x - 1, R, :]
            a2 = a[x, pl.ds(9, Y), :] - a[x, pl.ds(7, Y), :]
            return a1, a2, a3

        def edge(x):
            a1, a2, a3 = vectors(rho, x, slope(rho[x, R, :]))
            b1, b2, b3 = vectors(sig, x, slope(sig[x, R, :]))
            c2 = a3 * b1 - a1 * b3
            c3 = a1 * b2 - a2 * b1
            u1[x - 1] = b2 * c3 - b3 * c2
            v1[x - 1] = c2 * a3 - c3 * a2

        def pass1(i, acc, turn=lambda v: v):
            x = i + 2
            a1, a2, a3 = vectors(rho, x, da[i])
            b1, b2, b3 = vectors(sig, x, db[i])
            c1 = a2 * b3 - a3 * b2
            c2 = a3 * b1 - a1 * b3
            c3 = a1 * b2 - a2 * b1
            u1[i + 1] = b2 * c3 - b3 * c2
            v1[i + 1] = c2 * a3 - c3 * a2
            u2[i, R, :] = b3 * c1 - b1 * c3
            v2[i, R, :] = c3 * a1 - c1 * a3
            e3[i] = turn(b1 * c2 - b2 * c1)
            f3[i] = turn(c1 * a2 - c2 * a1)
            for s in range(2):
                at = pl.ds(7 + s * (Y + 1), 1)
                u2[i, at, :] = rim2[s, 0, pl.ds(i, 1), :]
                v2[i, at, :] = rim2[s, 1, pl.ds(i, 1), :]
            if late:
                return acc + fold(c1 * c1 + c2 * c2 + c3 * c3)
            c1s[i] = c1
            c2s[i] = c2
            c3s[i] = c3
            return acc

        def zadj(i, m):
            for a in (e3, f3):
                a[i:i + m] = jnp.dot(
                    split(a[i:i + m].reshape(m * Y, Z)), wts[:, Z:2 * Z],
                    preferred_element_type=F32).reshape(m, Y, Z)

        with scope("pass1"):
            csq = z8
            done = 1
            for i in range(1, X - 1):
                csq = pass1(i, csq)
                if i - done == GROUP or i == X - 2:
                    last = i + 1 if i == X - 2 else i
                    zadj(done, last - done)
                    done = last
        with scope("xrimwait"):
            xrims_wait(k)
        for s in range(2):
            pls = pl.ds(s * (X + 2), 2)
            if k == 0:
                rho[pls, R, :] = xrecv[0, s, 0]
                sig[pls, R, :] = xrecv[0, s, 1]
            else:
                rho[pls, R, :] = jnp.minimum(jnp.maximum(
                    rho[pls, R, :] - step_r * xrecv[k, s, 0], xrecv[3, s, 0]), xrecv[3, s, 1])
                sig[pls, R, :] = sig[pls, R, :] - step_s * xrecv[k, s, 1]
        rims_sent(k)
        if k == 1:
            rims_sent(BOUNDS)
        with scope("edge"):
            edge(1)
            edge(X + 2)
            csq = pass1(0, csq, slope)
            csq = pass1(X - 1, csq, slope)

        with scope("pwwait"):
            if k == 0:
                a, b = pw_wait(0)
                before[...] = (tscale * xscale) * a
                zsum[...] = tscale * (b + zown)
            else:
                a, b = pw_wait(k)
                before[...] = before[...] - (step_s * (tscale * xscale)) * a
                zsum[...] = zsum[...] - (step_s * (tscale * xscale)) * (b + wg)
        start = (float(N) - i0) * before[...] + zsum[...]

        def pass2(i, carry):
            pref, back, acc, nrho, nsig = carry
            v = sig[i + 2, R, :]
            pref = pref + (tscale * xscale) * v
            rt = pref - t[i]
            adj_s = (v1[i] - v1[i + 2]) + (v2[i, pl.ds(7, Y), :] - v2[i, pl.ds(9, Y), :]) - f3[i]
            gs = back + adj_s
            back = back - rt
            adj_r = (u1[i] - u1[i + 2]) + (u2[i, pl.ds(7, Y), :] - u2[i, pl.ds(9, Y), :]) - e3[i]
            gr = lin[i] - gp[i] + adj_r
            grho[i] = gr
            gsig[i] = gs
            if late:
                acc = acc + fold(rt * rt)
            else:
                miss[i] = rt
            nrho = nrho + fold(gr * gr)
            nsig = nsig + fold(gs * gs)
            if k < ITERS - 1:
                gather(0, 0, i, gr)
                gather(0, 1, i, gs)
            return pref, back, acc, nrho, nsig

        with scope("pass2"):
            carry = (before[...], start, z8, z8, z8)
            for i in range(X):
                carry = pass2(i, carry)
            _, _, acc, nrho, nsig = carry
        def objective(acc, psq, csq):
            return (0.5 / cells) * ((1.0 / (tscale * tscale)) * acc + psq + (BETA / 16.0) * csq)

        lane = lax.broadcasted_iota(jnp.int32, (1, Z), 1)

        def total(v):
            return jnp.sum(jnp.sum(v, axis=0, keepdims=True), axis=1, keepdims=True)

        row = jnp.where(lane < 1, total(nrho), total(nsig))
        if k > 0:
            row = jnp.where(lane < 2, row, total(past))
        if late:
            row = jnp.where(lane < 3, row, total(objective(acc, psq, csq)))
        nsend[k, 0:1] = row
        nrecv[k, n - 1:n] = row
        with scope("nstart"):
            n_start(k)
        if k < ITERS - 1:
            with scope("rimstart"):
                corners()
                rims_start(k + 1)

            def weigh(i, carry):
                pg, wg = carry
                gs = gsig[i]
                return pg + gs, wg + (float(N) - i0 - i.astype(F32)) * gs

            with scope("weigh"):
                pg, wg = lax.fori_loop(0, X, weigh, (zero, zero), unroll=8)
                pwsend[0] = pg
                pwsend[1] = wg
                pw_start(k + 1)

            def squares(i, carry):
                acc, csq = carry
                c1, c2, c3, rt = c1s[i], c2s[i], c3s[i], miss[i]
                return acc + fold(rt * rt), csq + fold(c1 * c1 + c2 * c2 + c3 * c3)

            with scope("dg"):
                dg[...] = zslope(gsig[...].reshape(X * Y, Z)).reshape(X, Y, Z)
            with scope("squares"):
                acc, csq = lax.fori_loop(0, X, squares, (z8, z8), unroll=4)
            if k > 0:
                with scope("psq"):
                    psq = pressure(product(rho[inner[0], R, :].reshape(X * Y, Z), slice(2 * Z, 3 * Z)))
            past = objective(acc, psq, csq)
            if k == 0:
                with scope("zonewait"):
                    yrims_wait(BOUNDS)
                    xrims_wait(BOUNDS)
                for s in range(2):
                    for slot in range(2):
                        yrecv[BOUNDS, s, 0, slot], yrecv[BOUNDS, s, 1, slot] = limits(zyrecv[s, slot])
                    xrecv[BOUNDS, s, 0], xrecv[BOUNDS, s, 1] = limits(zxrecv[s])
                for sx, sy in sides:
                    crecv[BOUNDS, sx, sy, 0:1, :], crecv[BOUNDS, sx, sy, 1:2, :] = limits(zcrecv[sx, sy, 0:1, :])
        with scope("nwait"):
            tot = n_wait(k)
        steps = (ETA / gain) * lax.rsqrt(tot / (gain * gain * cells) + EPSILON)
        step_r = jnp.broadcast_to(steps[0:1, 0:1], (1, Z))
        step_s = jnp.broadcast_to(steps[0:1, 1:2], (1, Z))
        if k > 0:
            stat[k - 1:k, :] = jnp.broadcast_to(tot[0:1, 2:3], (1, Z))
        if late:
            stat[k:k + 1, :] = jnp.broadcast_to(tot[0:1, 3:4], (1, Z))
            stat[ITERS:ITERS + 1, :] = step_r
            stat[ITERS + 1:ITERS + 2, :] = step_s


def finish(both, grad, lim, stat, rho_o, sig_o, obj_o, rho_b, sig_b, obj, sems):
    X, Y, Z = rho_b.shape
    R = pl.ds(8, Y)
    seen = stat[...]
    for k in range(ITERS):
        obj[k] = seen[k, 0]
    copies = [pltpu.make_async_copy(obj, obj_o, sems.at[0])]
    copies[0].start()
    step_r = stat[ITERS:ITERS + 1, :]
    step_s = stat[ITERS + 1:ITERS + 2, :]

    def move(i, carry):
        rho_b[i] = jnp.minimum(jnp.maximum(both[0, i + 2, R, :] - step_r * grad[0, i], lim[0, i]), lim[1, i])
        sig_b[i] = both[1, i + 2, R, :] - step_s * grad[1, i]
        return carry

    parts = 4
    for c in range(parts):
        lax.fori_loop(c * X // parts, (c + 1) * X // parts, move, 0, unroll=4)
        rows = pl.ds(c * X // parts, X // parts)
        for f, (a, b) in enumerate(((rho_b, rho_o), (sig_b, sig_o))):
            copies.append(pltpu.make_async_copy(a.at[rows], b.at[rows], sems.at[1 + 2 * c + f]))
            copies[-1].start()
    for c in copies:
        c.wait()


def local(density, slowness, pressure_obs, time_obs, zone_map, zone_low, zone_high):
    X, Y, Z = density.shape
    nx, ny = lax.axis_size("gx"), lax.axis_size("gy")
    assert Z <= 256
    V = pltpu.VMEM
    cube = (X, Y, Z)
    padded = (2, X + 4, Y + 16, Z)
    dma = pltpu.SemaphoreType.DMA
    anyspace = pl.BlockSpec(memory_space=pl.ANY)
    zones = zone_low.shape[0]
    scratch = [
        pltpu.SMEM((zones,), F32), pltpu.SMEM((zones,), F32),
        V(cube, F32), V(cube, F32),
        V(cube, jnp.int32), V(cube, F32), V(cube, F32),
        V((X + 2, Y, Z), F32), V((X + 2, Y, Z), F32), V((X, Y + 16, Z), F32), V((X, Y + 16, Z), F32),
        V(cube, F32), V(cube, F32), V(cube, F32), V(cube, F32),
        V(cube, F32), V(cube, F32), V(cube, F32), V(cube, F32), V(cube, F32), V((4 * X, Z), F32),
        V((2 * Z, 3 * Z), BF16), V((2 * Z, Z), BF16),
        V((2, 2, X, Z), jnp.int32), V((2, 2, X, Z), jnp.int32), V((2, 2, Y, Z), jnp.int32),
        V((2, 2, 8, Z), jnp.int32), V((2, 2, 8, Z), jnp.int32),
        V((2, 2, 3, X + 16, Z), F32), V((2, 2, X, Z), F32),
        V((2, 2, 2, 2, X, Z), F32), V((4, 2, 2, 2, X, Z), F32), V((4, 2, 2, 2, Y, Z), F32),
        V((2, 2, 8, Z), F32), V((4, 2, 2, 8, Z), F32),
        V((2, Y, Z), F32), V((ITERS, nx - 1, Y, Z), F32), V((Y, Z), F32), V((Y, Z), F32),
        V((ITERS, 8, Z), F32), V((ITERS, nx * ny, Z), F32),
        dma((7,)), dma((2, 2)), dma((3, 2)), dma((2, 2)), dma((3, 2)),
        dma((2, 2, 2)), dma((3, 2, 2)), dma((1,)), dma((2,)),
        dma((1,)), dma((2,)),
    ]
    inside = pl.BlockSpec(memory_space=pltpu.VMEM)
    state = pl.pallas_call(
        functools.partial(kernel, nx, ny),
        out_shape=(V(padded, F32), V((2,) + cube, F32), V((2,) + cube, F32), V((8, Z), F32)),
        in_specs=[pl.BlockSpec(memory_space=pltpu.HBM)] * 7,
        out_specs=(inside,) * 4,
        scratch_shapes=scratch,
        compiler_params=pltpu.CompilerParams(
            collective_id=0, has_side_effects=True, vmem_limit_bytes=48 * 1024 * 1024),
        name="inversion",
    )(zone_low, zone_high, density, slowness, pressure_obs, time_obs, zone_map)
    return pl.pallas_call(
        finish,
        out_shape=(
            jax.ShapeDtypeStruct(cube, F32),
            jax.ShapeDtypeStruct(cube, F32),
            jax.ShapeDtypeStruct((ITERS,), F32),
        ),
        in_specs=[inside] * 4,
        out_specs=(anyspace,) * 3,
        scratch_shapes=[V(cube, F32), V(cube, F32), pltpu.SMEM((ITERS,), F32), dma((9,))],
        compiler_params=pltpu.CompilerParams(vmem_limit_bytes=20 * 1024 * 1024),
        name="finish",
    )(*(pltpu.with_memory_space_constraint(a, pltpu.VMEM) for a in state))


def solution(mesh):
    cube = P("gx", "gy", None)
    return jax.shard_map(
        local,
        mesh=mesh,
        in_specs=(cube,) * 5 + (P(), P()),
        out_specs=(cube, cube, P()),
        check_vma=False,
    )
```

```python
import functools
import math

import jax
import jax.numpy as jnp
from jax import lax
from jax.experimental import pallas as pl
from jax.experimental.pallas import tpu as pltpu
from jax.sharding import PartitionSpec as P

ITERS = 3
BETA = 1.0
ETA = 0.5
EPSILON = 1e-06
MESH = pl.DeviceIdType.MESH
F32 = jnp.float32
BF16 = jnp.bfloat16
BOUNDS = 3
BANK = (0, 1, 0, 2)
UNROLL2 = 2
GROUP = 8
scope = jax.named_scope


def split(v):
    hi = v.astype(BF16)
    lo = (v - hi.astype(F32)).astype(BF16)
    return jnp.concatenate([hi, lo], axis=-1)


def kernel(
    nx, ny,
    zlow_h, zhigh_h, rho_h, sig_h, p_h, t_h, zone_h,
    both, grad, lim, stat,
    zlow, zhigh, p, t, zone, gp, lin,
    u1, v1, u2, v2, e3, f3, da, db, dg, miss, c1s, c2s, c3s, dedge, wts, ltab,
    zsend, zyrecv, zxrecv, zcsend, zcrecv,
    rim, rim2, ysend, yrecv, xrecv, csend, crecv, pwsend, pwrecv, before, zsum, nsend, nrecv,
    insem, ys, yr, xs_, xr, cs, cr, ps, pr, ns, nr,
):
    X, Y, Z = p.shape
    rho, sig = both.at[0], both.at[1]
    grho, gsig = grad.at[0], grad.at[1]
    low, high = lim.at[0], lim.at[1]
    mx, my = lax.axis_index("gx"), lax.axis_index("gy")
    n = nx * ny
    N = nx * X
    cells = float(N * ny * Y * Z)
    zscale = 1.0 / math.sqrt(Z)
    xscale = 1.0 / math.sqrt(N)
    gain = 16.0 / BETA
    tscale = gain * xscale
    R = pl.ds(8, Y)
    XI = pl.ds(8, X)
    i0 = (mx * X).astype(F32)

    inner = (pl.ds(2, X), R)
    loads = [
        pltpu.make_async_copy(sig_h, sig.at[inner], insem.at[0]),
        pltpu.make_async_copy(rho_h, rho.at[inner], insem.at[1]),
        pltpu.make_async_copy(t_h, t, insem.at[2]),
        pltpu.make_async_copy(zone_h, zone, insem.at[3]),
        pltpu.make_async_copy(p_h, p, insem.at[4]),
        pltpu.make_async_copy(zlow_h, zlow, insem.at[5]),
        pltpu.make_async_copy(zhigh_h, zhigh, insem.at[6]),
    ]
    for c in loads[:3]:
        c.start()
    barrier = pltpu.get_barrier_semaphore()

    has = {0: (mx > 0, my > 0), 1: (mx < nx - 1, my < ny - 1)}
    sides = [(sx, sy) for sx in range(2) for sy in range(2)]

    def other(dx, dy):
        tx = lax.rem(mx + dx, nx) if dx else mx
        ty = lax.rem(my + dy, ny) if dy else my
        return tx, ty

    pairs = [(dx, dy) for dx in range(nx) for dy in range(ny)][1:]
    lines = [(dx, dy) for dx, dy in pairs if dx == 0 or dy == 0]
    for dx, dy in lines:
        pl.semaphore_signal(barrier, inc=1, device_id=other(dx, dy), device_id_type=MESH)
    count = len(lines)
    for sx, sy in sides:
        diagonal = jnp.logical_and(has[sx][0], has[sy][1])
        count = count + diagonal.astype(jnp.int32)

        @pl.when(diagonal)
        def _():
            pl.semaphore_signal(
                barrier, inc=1, device_id=(mx + (2 * sx - 1), my + (2 * sy - 1)), device_id_type=MESH)


    def blank(ref, at, value):
        ref[at] = jnp.full(ref.shape[len(at):], value, ref.dtype)

    for s in range(2):
        @pl.when(jnp.logical_not(has[s][1]))
        def _():
            blank(zyrecv, (s,), -1)
            for r in range(ITERS):
                blank(yrecv, (r, s), 0.0)

        @pl.when(jnp.logical_not(has[s][0]))
        def _():
            blank(zxrecv, (s,), -1)
            for r in range(ITERS):
                blank(xrecv, (r, s), 0.0)
    for sx, sy in sides:
        @pl.when(jnp.logical_not(jnp.logical_and(has[sx][0], has[sy][1])))
        def _():
            blank(zcrecv, (sx, sy), -1)
            for r in range(ITERS):
                blank(crecv, (r, sx, sy), 0.0)

    def ycopy(r, s):
        b = 1 if r == BOUNDS else 0
        return pltpu.make_async_remote_copy(
            src_ref=zsend.at[s] if b else ysend.at[0, s],
            dst_ref=zyrecv.at[1 - s] if b else yrecv.at[r, 1 - s],
            send_sem=ys.at[b, s], recv_sem=yr.at[BANK[r], 1 - s],
            device_id=(mx, my + (2 * s - 1)), device_id_type=MESH)

    def xcopy(r, s):
        b = 1 if r == BOUNDS else 0
        planes = pl.ds(s * (X - 2), 2)
        if r == 0:
            src = both.at[:, pl.ds(2 + s * (X - 2), 2), R]
        else:
            src = zone.at[planes] if b else grad.at[:, planes]
        return pltpu.make_async_remote_copy(
            src_ref=src, dst_ref=zxrecv.at[1 - s] if b else xrecv.at[r, 1 - s],
            send_sem=xs_.at[b, s], recv_sem=xr.at[BANK[r], 1 - s],
            device_id=(mx + (2 * s - 1), my), device_id_type=MESH)

    def ccopy(r, sx, sy):
        b = 1 if r == BOUNDS else 0
        src = zcsend.at[sx, sy, pl.ds(0, 1)] if b else csend.at[sx, sy, pl.ds(0, 2)]
        dst = zcrecv.at[1 - sx, 1 - sy, pl.ds(0, 1)] if b else crecv.at[r, 1 - sx, 1 - sy, pl.ds(0, 2)]
        return pltpu.make_async_remote_copy(
            src_ref=src, dst_ref=dst,
            send_sem=cs.at[b, sx, sy], recv_sem=cr.at[BANK[r], 1 - sx, 1 - sy],
            device_id=(mx + (2 * sx - 1), my + (2 * sy - 1)), device_id_type=MESH)

    def rims_start(r):
        for sx, sy in sides:
            @pl.when(jnp.logical_and(has[sx][0], has[sy][1]))
            def _():
                ccopy(r, sx, sy).start()
        for s in range(2):
            @pl.when(has[s][1])
            def _():
                ycopy(r, s).start()

            @pl.when(has[s][0])
            def _():
                xcopy(r, s).start()

    def yrims_wait(r):
        for s in range(2):
            @pl.when(has[s][1])
            def _():
                ycopy(r, 1 - s).wait_recv()
        for sx, sy in sides:
            @pl.when(jnp.logical_and(has[sx][0], has[sy][1]))
            def _():
                ccopy(r, 1 - sx, 1 - sy).wait_recv()

    def xrims_wait(r):
        for s in range(2):
            @pl.when(has[s][0])
            def _():
                xcopy(r, 1 - s).wait_recv()

    def rims_sent(r):
        for s in range(2):
            @pl.when(has[s][1])
            def _():
                ycopy(r, s).wait_send()

            @pl.when(has[s][0])
            def _():
                xcopy(r, s).wait_send()
        for sx, sy in sides:
            @pl.when(jnp.logical_and(has[sx][0], has[sy][1]))
            def _():
                ccopy(r, sx, sy).wait_send()

    def pw_start(r):
        for dx in range(1, nx):
            tx, _ = other(dx, 0)
            pltpu.make_async_remote_copy(
                src_ref=pwsend.at[jnp.where(tx > mx, 0, 1)], dst_ref=pwrecv.at[r, dx - 1],
                send_sem=ps.at[0], recv_sem=pr.at[r % 2],
                device_id=(tx, my), device_id_type=MESH).start()

    def pw_wait(r):
        slots = pwrecv.at[r, pl.ds(0, nx - 1)]
        every = pltpu.make_async_remote_copy(
            src_ref=slots, dst_ref=slots, send_sem=ps.at[0], recv_sem=pr.at[r % 2],
            device_id=other(1, 0), device_id_type=MESH)
        every.wait_recv()
        every.wait_send()
        a = jnp.zeros((Y, Z), F32)
        b = jnp.zeros((Y, Z), F32)
        for dx in range(1, nx):
            w = jnp.where(dx <= mx, 1.0, 0.0)
            v = pwrecv[r, dx - 1]
            a = a + v * w
            b = b + v * (1.0 - w)
        return a, b

    def n_start(r):
        for d, (dx, dy) in enumerate(pairs):
            pltpu.make_async_remote_copy(
                src_ref=nsend.at[r, pl.ds(0, 1)], dst_ref=nrecv.at[r, pl.ds(d, 1)],
                send_sem=ns.at[0], recv_sem=nr.at[r % 2],
                device_id=other(dx, dy), device_id_type=MESH).start()

    def n_wait(r):
        rows = nrecv.at[r, pl.ds(0, n - 1)]
        every = pltpu.make_async_remote_copy(
            src_ref=rows, dst_ref=rows, send_sem=ns.at[0], recv_sem=nr.at[r % 2],
            device_id=other(0, 1), device_id_type=MESH)
        every.wait_recv()
        every.wait_send()
        return jnp.sum(nrecv[r], axis=0, keepdims=True)

    def fold(v):
        out = v[0:8]
        for k in range(8, v.shape[0], 8):
            out = out + v[k:k + 8]
        return out

    def gather(b, f, x, v):
        row = pl.ds(x, 1)
        ysend[b, 0, f, 0, row, :] = v[0:1]
        ysend[b, 0, f, 1, row, :] = v[1:2]
        ysend[b, 1, f, 0, row, :] = v[Y - 1:Y]
        ysend[b, 1, f, 1, row, :] = v[Y - 2:Y - 1]

    def corners():
        for f in range(2):
            for sx, sy in sides:
                csend[sx, sy, f:f + 1, :] = ysend[0, sy, f, 0, sx * (X - 1):sx * (X - 1) + 1, :]

    def slope(v):
        lane = lax.broadcasted_iota(jnp.int32, v.shape, 1)
        up = jnp.where(lane < Z - 1, pltpu.roll(v, Z - 1, 1), 0.0)
        return up - jnp.where(lane > 0, pltpu.roll(v, 1, 1), 0.0)

    zero = jnp.zeros((Y, Z), F32)
    z8 = jnp.zeros((8, Z), F32)

    with scope("load02"):
        loads[0].wait()
        loads[2].wait()
        for c in loads[3:]:
            c.start()

    def sums(x, carry):
        a, b, c = carry
        v = sig[x + 2, R, :]
        gather(0, 1, x, v)
        weight = float(N) - i0 - x.astype(F32)
        return a + v, b + weight * v, c + t[x]

    psum_, wsum, tsum = lax.fori_loop(0, X, sums, (zero, zero, zero), unroll=4)
    zown = xscale * wsum - tsum
    pwsend[0] = psum_
    pwsend[1] = zown
    loads[1].wait()

    def copy_rho(x, carry):
        gather(0, 0, x, rho[x + 2, R, :])
        return carry

    lax.fori_loop(0, X, copy_rho, 0, unroll=4)
    corners()
    with scope("barrier"):
        pl.semaphore_wait(barrier, count)
    with scope("rims0start"):
        rims_start(0)
        pw_start(0)

    for c in loads[3:]:
        c.wait()

    def limits(ids):
        lo = jnp.zeros(ids.shape, F32)
        hi = jnp.zeros(ids.shape, F32)
        for k in range(zlow.shape[0]):
            hit = ids == k
            lo = jnp.where(hit, zlow[k], lo)
            hi = jnp.where(hit, zhigh[k], hi)
        return lo, hi

    def bounds(x, carry):
        ids = zone[x]
        lo, hi = limits(ids)
        row = pl.ds(x, 1)
        for s in range(2):
            for slot in range(2):
                at = s * (Y - 1) + (1 - 2 * s) * slot
                zsend[s, slot, row, :] = ids[at:at + 1]
        low[x] = lo
        high[x] = hi
        t[x] = tscale * t[x]
        gather(1, 0, x, lo)
        gather(1, 1, x, hi)
        return carry

    with scope("bounds"):
        lax.fori_loop(0, X, bounds, 0, unroll=2)
        for sx, sy in sides:
            zcsend[sx, sy, 0:1, :] = zsend[sy, 0, sx * (X - 1):sx * (X - 1) + 1, :]

    ri = lax.broadcasted_iota(jnp.int32, (Z, Z), 0)
    ci = lax.broadcasted_iota(jnp.int32, (Z, Z), 1)
    m = (Z - jnp.maximum(ri, ci)).astype(F32).astype(BF16)
    u = jnp.where(ri <= ci, 1.0, 0.0).astype(BF16)
    band = jnp.where(ri == ci + 1, 1.0, jnp.where(ri == ci - 1, -1.0, 0.0)).astype(BF16)
    l = jnp.where(ri >= ci, 1.0, 0.0).astype(BF16)
    for half in (slice(0, Z), slice(Z, 2 * Z)):
        wts[half, 0:Z] = m
        wts[half, Z:2 * Z] = band
        wts[half, 2 * Z:3 * Z] = u
        ltab[half] = l

    with scope("pback"):
        v = p[...].reshape(X * Y, Z)
        out = jnp.dot(split(v), ltab[...], preferred_element_type=F32)
        gp[...] = (out * (gain * zscale)).reshape(X, Y, Z)

    def product(v, columns):
        rows = v.shape[0] // 2
        return jnp.concatenate([
            jnp.dot(split(v[h * rows:(h + 1) * rows]), wts[:, columns], preferred_element_type=F32)
            for h in range(2)], axis=0)

    def zslope(v):
        return product(v, slice(Z, 2 * Z))

    def zlin(v, columns):
        out = product(v.reshape(X * Y, Z), slice(0, columns * Z))
        lin[...] = (out[:, 0:Z] * (gain * zscale * zscale)).reshape(X, Y, Z)
        da[...] = out[:, Z:2 * Z].reshape(X, Y, Z)
        return pressure(out[:, 2 * Z:3 * Z]) if columns > 2 else None

    def pressure(v):
        rp = zscale * v - p[...].reshape(X * Y, Z)
        return fold(rp * rp)

    def edges():
        dedge[...] = slope(jnp.concatenate(
            [rim[f, s, 1, XI, :] for f in range(2) for s in range(2)], axis=0))

    def set_rows(x):
        for f, a in ((0, rho), (1, sig)):
            for s in range(2):
                a[x + 2, 7 + s * (Y + 1):8 + s * (Y + 1), :] = rim[f, s, 1, 8 + x:9 + x, :]

    def set_corners():
        for f, a in ((0, rho), (1, sig)):
            for sx, sy in sides:
                a[1 + sx * (X + 1), pl.ds(7 + sy * (Y + 1), 1), :] = (
                    rim[f, sy, 1, 7 + sx * (X + 1):8 + sx * (X + 1), :])

    for k in range(ITERS):
        late = k == ITERS - 1
        if k == 0:
            with scope("zlin"):
                psq = zlin(rho[inner[0], R, :], 3)
                db[...] = zslope(sig[inner[0], R, :].reshape(X * Y, Z)).reshape(X, Y, Z)
        else:
            with scope("update"):
                v = jnp.minimum(jnp.maximum(rho[inner[0], R, :] - step_r * grho[...], low[...]), high[...])
                rho[inner[0], R, :] = v
                sig[inner[0], R, :] = sig[inner[0], R, :] - step_s * gsig[...]
                db[...] = db[...] - step_s * dg[...]
                psq = zlin(v, 3 if late else 2)
        if k == 0:
            with scope("yrimwait"):
                yrims_wait(0)
            with scope("rims3start"):
                rims_start(BOUNDS)
            for f, a in ((0, rho), (1, sig)):
                for s in range(2):
                    rim[f, s, 0, XI, :] = yrecv[0, s, f, 1]
                    rim[f, s, 1, XI, :] = yrecv[0, s, f, 0]
                    rim[f, s, 2, XI, :] = ysend[0, s, f, 0]
                    for sx in range(2):
                        rim[f, s, 1, 7 + sx * (X + 1):8 + sx * (X + 1), :] = crecv[0, sx, s, f:f + 1, :]
        else:
            with scope("yrimwait"):
                yrims_wait(k)
            for s in range(2):
                for row, slot in ((0, 1), (1, 0), (2, 0)):
                    gr = (ysend[0, s, 0, 0] if row == 2 else yrecv[k, s, 0, slot])
                    gs = (ysend[0, s, 1, 0] if row == 2 else yrecv[k, s, 1, slot])
                    lo = (ysend[1, s, 0, 0] if row == 2 else yrecv[3, s, 0, slot])
                    hi = (ysend[1, s, 1, 0] if row == 2 else yrecv[3, s, 1, slot])
                    rim[0, s, row, XI, :] = jnp.minimum(jnp.maximum(rim[0, s, row, XI, :] - step_r * gr, lo), hi)
                    rim[1, s, row, XI, :] = rim[1, s, row, XI, :] - step_s * gs
                for sx in range(2):
                    at = slice(7 + sx * (X + 1), 8 + sx * (X + 1))
                    rim[0, s, 1, at, :] = jnp.minimum(jnp.maximum(
                        rim[0, s, 1, at, :] - step_r * crecv[k, sx, s, 0:1, :],
                        crecv[3, sx, s, 0:1, :]), crecv[3, sx, s, 1:2, :])
                    rim[1, s, 1, at, :] = rim[1, s, 1, at, :] - step_s * crecv[k, sx, s, 1:2, :]
        with scope("setrows"):
            for x in range(X):
                set_rows(x)
            set_corners()
        with scope("edges"):
            edges()

        for s in range(2):
            def rimstep(base):
                def vec(f):
                    a1 = rim[f, s, 1, 9 + base:17 + base, :] - rim[f, s, 1, 7 + base:15 + base, :]
                    a2 = rim[f, s, 2 - 2 * s, 8 + base:16 + base, :] - rim[f, s, 2 * s, 8 + base:16 + base, :]
                    at = (2 * f + s) * X + base
                    return a1, a2, dedge[at:at + 8, :]
                a1, a2, a3 = vec(0)
                b1, b2, b3 = vec(1)
                c1 = a2 * b3 - a3 * b2
                c3 = a1 * b2 - a2 * b1
                rim2[s, 0, base:base + 8, :] = b3 * c1 - b1 * c3
                rim2[s, 1, base:base + 8, :] = c3 * a1 - c1 * a3

            for base in range(0, X, 8):
                rimstep(base)

        def vectors(a, x, a3):
            a1 = a[x + 1, R, :] - a[x - 1, R, :]
            a2 = a[x, pl.ds(9, Y), :] - a[x, pl.ds(7, Y), :]
            return a1, a2, a3

        def edge(x):
            a1, a2, a3 = vectors(rho, x, slope(rho[x, R, :]))
            b1, b2, b3 = vectors(sig, x, slope(sig[x, R, :]))
            c2 = a3 * b1 - a1 * b3
            c3 = a1 * b2 - a2 * b1
            u1[x - 1] = b2 * c3 - b3 * c2
            v1[x - 1] = c2 * a3 - c3 * a2

        def pass1(i, acc, turn=lambda v: v):
            x = i + 2
            a1, a2, a3 = vectors(rho, x, da[i])
            b1, b2, b3 = vectors(sig, x, db[i])
            c1 = a2 * b3 - a3 * b2
            c2 = a3 * b1 - a1 * b3
            c3 = a1 * b2 - a2 * b1
            u1[i + 1] = b2 * c3 - b3 * c2
            v1[i + 1] = c2 * a3 - c3 * a2
            u2[i, R, :] = b3 * c1 - b1 * c3
            v2[i, R, :] = c3 * a1 - c1 * a3
            e3[i] = turn(b1 * c2 - b2 * c1)
            f3[i] = turn(c1 * a2 - c2 * a1)
            for s in range(2):
                at = pl.ds(7 + s * (Y + 1), 1)
                u2[i, at, :] = rim2[s, 0, pl.ds(i, 1), :]
                v2[i, at, :] = rim2[s, 1, pl.ds(i, 1), :]
            if late:
                return acc + fold(c1 * c1 + c2 * c2 + c3 * c3)
            c1s[i] = c1
            c2s[i] = c2
            c3s[i] = c3
            return acc

        def zadj(i, m):
            for a in (e3, f3):
                a[i:i + m] = jnp.dot(
                    split(a[i:i + m].reshape(m * Y, Z)), wts[:, Z:2 * Z],
                    preferred_element_type=F32).reshape(m, Y, Z)

        with scope("pass1"):
            csq = z8
            done = 1
            for i in range(1, X - 1):
                csq = pass1(i, csq)
                if i - done == GROUP or i == X - 2:
                    last = i + 1 if i == X - 2 else i
                    zadj(done, last - done)
                    done = last
        with scope("xrimwait"):
            xrims_wait(k)
        for s in range(2):
            pls = pl.ds(s * (X + 2), 2)
            if k == 0:
                rho[pls, R, :] = xrecv[0, s, 0]
                sig[pls, R, :] = xrecv[0, s, 1]
            else:
                rho[pls, R, :] = jnp.minimum(jnp.maximum(
                    rho[pls, R, :] - step_r * xrecv[k, s, 0], xrecv[3, s, 0]), xrecv[3, s, 1])
                sig[pls, R, :] = sig[pls, R, :] - step_s * xrecv[k, s, 1]
        rims_sent(k)
        if k == 1:
            rims_sent(BOUNDS)
        with scope("edge"):
            edge(1)
            edge(X + 2)
            csq = pass1(0, csq, slope)
            csq = pass1(X - 1, csq, slope)

        with scope("pwwait"):
            if k == 0:
                a, b = pw_wait(0)
                before[...] = (tscale * xscale) * a
                zsum[...] = tscale * (b + zown)
            else:
                a, b = pw_wait(k)
                before[...] = before[...] - (step_s * (tscale * xscale)) * a
                zsum[...] = zsum[...] - (step_s * (tscale * xscale)) * (b + wg)
        start = (float(N) - i0) * before[...] + zsum[...]

        def pass2(i, carry):
            pref, back, acc, nrho, nsig = carry
            v = sig[i + 2, R, :]
            pref = pref + (tscale * xscale) * v
            rt = pref - t[i]
            adj_s = (v1[i] - v1[i + 2]) + (v2[i, pl.ds(7, Y), :] - v2[i, pl.ds(9, Y), :]) - f3[i]
            gs = back + adj_s
            back = back - rt
            adj_r = (u1[i] - u1[i + 2]) + (u2[i, pl.ds(7, Y), :] - u2[i, pl.ds(9, Y), :]) - e3[i]
            gr = lin[i] - gp[i] + adj_r
            grho[i] = gr
            gsig[i] = gs
            if late:
                acc = acc + fold(rt * rt)
            else:
                miss[i] = rt
            nrho = nrho + fold(gr * gr)
            nsig = nsig + fold(gs * gs)
            if k < ITERS - 1:
                gather(0, 0, i, gr)
                gather(0, 1, i, gs)
            return pref, back, acc, nrho, nsig

        with scope("pass2"):
            carry = (before[...], start, z8, z8, z8)
            for i in range(X):
                carry = pass2(i, carry)
            _, _, acc, nrho, nsig = carry
        def objective(acc, psq, csq):
            return (0.5 / cells) * ((1.0 / (tscale * tscale)) * acc + psq + (BETA / 16.0) * csq)

        lane = lax.broadcasted_iota(jnp.int32, (1, Z), 1)

        def total(v):
            return jnp.sum(jnp.sum(v, axis=0, keepdims=True), axis=1, keepdims=True)

        row = jnp.where(lane < 1, total(nrho), total(nsig))
        if k > 0:
            row = jnp.where(lane < 2, row, total(past))
        if late:
            row = jnp.where(lane < 3, row, total(objective(acc, psq, csq)))
        nsend[k, 0:1] = row
        nrecv[k, n - 1:n] = row
        with scope("nstart"):
            n_start(k)
        if k < ITERS - 1:
            with scope("rimstart"):
                corners()
                rims_start(k + 1)

            def weigh(i, carry):
                pg, wg = carry
                gs = gsig[i]
                return pg + gs, wg + (float(N) - i0 - i.astype(F32)) * gs

            with scope("weigh"):
                pg, wg = lax.fori_loop(0, X, weigh, (zero, zero), unroll=8)
                pwsend[0] = pg
                pwsend[1] = wg
                pw_start(k + 1)

            def squares(i, carry):
                acc, csq = carry
                c1, c2, c3, rt = c1s[i], c2s[i], c3s[i], miss[i]
                return acc + fold(rt * rt), csq + fold(c1 * c1 + c2 * c2 + c3 * c3)

            with scope("dg"):
                dg[...] = zslope(gsig[...].reshape(X * Y, Z)).reshape(X, Y, Z)
            with scope("squares"):
                acc, csq = lax.fori_loop(0, X, squares, (z8, z8), unroll=4)
            if k > 0:
                with scope("psq"):
                    psq = pressure(product(rho[inner[0], R, :].reshape(X * Y, Z), slice(2 * Z, 3 * Z)))
            past = objective(acc, psq, csq)
            if k == 0:
                with scope("zonewait"):
                    yrims_wait(BOUNDS)
                    xrims_wait(BOUNDS)
                for s in range(2):
                    for slot in range(2):
                        yrecv[BOUNDS, s, 0, slot], yrecv[BOUNDS, s, 1, slot] = limits(zyrecv[s, slot])
                    xrecv[BOUNDS, s, 0], xrecv[BOUNDS, s, 1] = limits(zxrecv[s])
                for sx, sy in sides:
                    crecv[BOUNDS, sx, sy, 0:1, :], crecv[BOUNDS, sx, sy, 1:2, :] = limits(zcrecv[sx, sy, 0:1, :])
        with scope("nwait"):
            tot = n_wait(k)
        steps = (ETA / gain) * lax.rsqrt(tot / (gain * gain * cells) + EPSILON)
        step_r = jnp.broadcast_to(steps[0:1, 0:1], (1, Z))
        step_s = jnp.broadcast_to(steps[0:1, 1:2], (1, Z))
        if k > 0:
            stat[k - 1:k, :] = jnp.broadcast_to(tot[0:1, 2:3], (1, Z))
        if late:
            stat[k:k + 1, :] = jnp.broadcast_to(tot[0:1, 3:4], (1, Z))
            stat[ITERS:ITERS + 1, :] = step_r
            stat[ITERS + 1:ITERS + 2, :] = step_s


def finish(both, grad, lim, stat, rho_o, sig_o, obj_o, rho_b, sig_b, obj, sems):
    X, Y, Z = rho_b.shape
    R = pl.ds(8, Y)
    seen = stat[...]
    for k in range(ITERS):
        obj[k] = seen[k, 0]
    copies = [pltpu.make_async_copy(obj, obj_o, sems.at[0])]
    copies[0].start()
    step_r = stat[ITERS:ITERS + 1, :]
    step_s = stat[ITERS + 1:ITERS + 2, :]

    def move(i, carry):
        rho_b[i] = jnp.minimum(jnp.maximum(both[0, i + 2, R, :] - step_r * grad[0, i], lim[0, i]), lim[1, i])
        sig_b[i] = both[1, i + 2, R, :] - step_s * grad[1, i]
        return carry

    parts = 4
    for c in range(parts):
        lax.fori_loop(c * X // parts, (c + 1) * X // parts, move, 0, unroll=4)
        rows = pl.ds(c * X // parts, X // parts)
        for f, (a, b) in enumerate(((rho_b, rho_o), (sig_b, sig_o))):
            copies.append(pltpu.make_async_copy(a.at[rows], b.at[rows], sems.at[1 + 2 * c + f]))
            copies[-1].start()
    for c in copies:
        c.wait()


def local(density, slowness, pressure_obs, time_obs, zone_map, zone_low, zone_high):
    X, Y, Z = density.shape
    nx, ny = lax.axis_size("gx"), lax.axis_size("gy")
    assert Z <= 256
    V = pltpu.VMEM
    cube = (X, Y, Z)
    padded = (2, X + 4, Y + 16, Z)
    dma = pltpu.SemaphoreType.DMA
    anyspace = pl.BlockSpec(memory_space=pl.ANY)
    zones = zone_low.shape[0]
    scratch = [
        pltpu.SMEM((zones,), F32), pltpu.SMEM((zones,), F32),
        V(cube, F32), V(cube, F32),
        V(cube, jnp.int32), V(cube, F32), V(cube, F32),
        V((X + 2, Y, Z), F32), V((X + 2, Y, Z), F32), V((X, Y + 16, Z), F32), V((X, Y + 16, Z), F32),
        V(cube, F32), V(cube, F32), V(cube, F32), V(cube, F32),
        V(cube, F32), V(cube, F32), V(cube, F32), V(cube, F32), V(cube, F32), V((4 * X, Z), F32),
        V((2 * Z, 3 * Z), BF16), V((2 * Z, Z), BF16),
        V((2, 2, X, Z), jnp.int32), V((2, 2, X, Z), jnp.int32), V((2, 2, Y, Z), jnp.int32),
        V((2, 2, 8, Z), jnp.int32), V((2, 2, 8, Z), jnp.int32),
        V((2, 2, 3, X + 16, Z), F32), V((2, 2, X, Z), F32),
        V((2, 2, 2, 2, X, Z), F32), V((4, 2, 2, 2, X, Z), F32), V((4, 2, 2, 2, Y, Z), F32),
        V((2, 2, 8, Z), F32), V((4, 2, 2, 8, Z), F32),
        V((2, Y, Z), F32), V((ITERS, nx - 1, Y, Z), F32), V((Y, Z), F32), V((Y, Z), F32),
        V((ITERS, 8, Z), F32), V((ITERS, nx * ny, Z), F32),
        dma((7,)), dma((2, 2)), dma((3, 2)), dma((2, 2)), dma((3, 2)),
        dma((2, 2, 2)), dma((3, 2, 2)), dma((1,)), dma((2,)),
        dma((1,)), dma((2,)),
    ]
    inside = pl.BlockSpec(memory_space=pltpu.VMEM)
    state = pl.pallas_call(
        functools.partial(kernel, nx, ny),
        out_shape=(V(padded, F32), V((2,) + cube, F32), V((2,) + cube, F32), V((8, Z), F32)),
        in_specs=[pl.BlockSpec(memory_space=pltpu.HBM)] * 7,
        out_specs=(inside,) * 4,
        scratch_shapes=scratch,
        compiler_params=pltpu.CompilerParams(
            collective_id=0, has_side_effects=True, vmem_limit_bytes=48 * 1024 * 1024),
        name="inversion",
    )(zone_low, zone_high, density, slowness, pressure_obs, time_obs, zone_map)
    return pl.pallas_call(
        finish,
        out_shape=(
            jax.ShapeDtypeStruct(cube, F32),
            jax.ShapeDtypeStruct(cube, F32),
            jax.ShapeDtypeStruct((ITERS,), F32),
        ),
        in_specs=[inside] * 4,
        out_specs=(anyspace,) * 3,
        scratch_shapes=[V(cube, F32), V(cube, F32), pltpu.SMEM((ITERS,), F32), dma((9,))],
        compiler_params=pltpu.CompilerParams(vmem_limit_bytes=20 * 1024 * 1024),
        name="finish",
    )(*(pltpu.with_memory_space_constraint(a, pltpu.VMEM) for a in state))


def solution(mesh):
    cube = P("gx", "gy", None)
    return jax.shard_map(
        local,
        mesh=mesh,
        in_specs=(cube,) * 5 + (P(), P()),
        out_specs=(cube, cube, P()),
        check_vma=False,
    )
```
